32 devices in a mesh: dp: 2 (over core), tensor: 16 (over z, y, x).
Axes of the slice: x: 2, y: 2, z: 4, core: 2. Of those that a mesh axis runs over, the one named last changes fastest.
Arguments:
- resid_stream: bfloat16 [512, 4608], P(('dp', 'tensor')), parts along dimension 0, may hold values from -120 to 120, as said below
- pre_gain: float32 [4608], replicated, may hold values from 0.5 to 1.5
- w_gate: bfloat16 [4608, 6144], P(None, 'tensor'), may hold values from -0.09375 to 0.09375
- w_up: bfloat16 [4608, 6144], P(None, 'tensor'), may hold values from -0.09375 to 0.09375
- w_down: bfloat16 [6144, 4608], P('tensor'), may hold values from -0.078125 to 0.078125
- post_gain: float32 [4608], replicated, may hold values from 0.5 to 1.5
Outputs:
- resid_out: bfloat16 [512, 4608], P(('dp', 'tensor')), parts along dimension 0
The draws below stay inside these ranges and needn't reach their ends.
There are 2 independent parts, one for each index of `dp`. The reference program is written for one: setup_inputs(seed, part) draws one part's arguments, and reference() takes and returns one part's arrays. A program takes and returns all parts, laid end to end along the dimension named above; an argument that names none is the same for every part. Nothing has to cross between parts.
Inputs may be any that keep to these rules, and one draw needn't show every extreme that they name: `resid_stream`: entries are real-valued.
All inputs are finite; a program needn't handle non-finite values.
Results may differ from the reference program's by a relative error of at most 0.0029.
Values may be sent and summed in bfloat16 or wider, within the bound.
A program may use at most 128 MiB of HBM per device.

```python
import jax
import jax.numpy as jnp
from jax import lax

D = 4608
TOKENS = 256
FF_WIN = 6144


def draw_resid_stream(key, part):
    keys = jax.random.split(jax.random.fold_in(key, 17), 3)
    base = jnp.clip(jax.random.normal(keys[0], (TOKENS, D), jnp.float32), -4.0, 4.0)
    row_scale = jnp.exp(jax.random.uniform(keys[1], (TOKENS, 1), jnp.float32) * 2.302585)
    col_scale = jnp.exp(jax.random.uniform(keys[2], (1, D), jnp.float32, minval=-1.15, maxval=1.15))
    values = base * row_scale * col_scale
    return jnp.clip(values, -120.0, 120.0).astype(jnp.bfloat16)


def level_of(rng, shape, pieces, low, high):
    level = 1.0
    for position, shards_of in pieces:
        draws = jax.random.uniform(jax.random.fold_in(jax.random.fold_in(rng, 6), position), (shards_of,), jnp.float32, low / len(pieces), high / len(pieces))
        level = level * jnp.repeat(jnp.exp(draws), shape[position] // shards_of).reshape((-1,) + (1,) * (len(shape) - 1 - position))
    return level


def bell_draw(key, dims, scale, limit, pieces=(), kind=jnp.bfloat16):
    result = jax.random.normal(key, dims, jnp.float32) * scale
    if len(pieces) > 0:
        result = level_of(key, dims, pieces, -0.22, 0.18) * result
    return jnp.clip(result, min=-limit, max=limit).astype(kind)


def setup_inputs(seed: int = 0, part: int = 0) -> dict:
    key_list = jax.random.split(jax.random.key(seed), 7)
    part_keys = jax.random.split(jax.random.fold_in(key_list[6], part), 7)
    resid_stream = draw_resid_stream(jax.random.fold_in(jax.random.fold_in(key_list[6], part), 71), part)
    pre_gain = jnp.clip(1.0 + 0.1 * jax.random.normal(key_list[1], (D,), jnp.float32), 0.5, 1.5)
    w_gate = bell_draw(key_list[2], (D, FF_WIN), D ** -0.5, 0.09375, ((1, 16),))
    w_up = bell_draw(key_list[3], (D, FF_WIN), D ** -0.5, 0.09375, ((1, 16),))
    w_down = bell_draw(key_list[4], (FF_WIN, D), FF_WIN ** -0.5, 0.078125, ((0, 16),))
    post_gain = jnp.clip(1.0 + 0.1 * jax.random.normal(key_list[5], (D,), jnp.float32), 0.5, 1.5)
    return {"resid_stream": resid_stream, "pre_gain": pre_gain, "w_gate": w_gate, "w_up": w_up, "w_down": w_down, "post_gain": post_gain}


norm_eps = 1e-06

def rms_scale(values):
    return values * lax.rsqrt(lax.optimization_barrier(jnp.mean(values * values, axis=-1, keepdims=True)) + norm_eps)

def reference(resid_stream, pre_gain, w_gate, w_up, w_down, post_gain):
    stream = resid_stream.astype(jnp.float32)
    normed = (rms_scale(stream) * pre_gain.astype(jnp.float32)).astype(jnp.bfloat16)
    gate_out = jnp.dot(normed, w_gate, preferred_element_type=jnp.float32)
    up_out = jnp.dot(normed, w_up, preferred_element_type=jnp.float32)
    hidden = (jax.nn.gelu(gate_out, approximate=True) * up_out).astype(jnp.bfloat16)
    block_out = jnp.dot(hidden, w_down, preferred_element_type=jnp.float32)
    post = (rms_scale(block_out) * post_gain.astype(jnp.float32)).astype(jnp.bfloat16)
    post = lax.optimization_barrier(post)
    return (stream + post.astype(jnp.float32)).astype(jnp.bfloat16)
```

```python
import functools

import jax
import jax.numpy as jnp
from jax import lax
from jax.experimental import pallas as pl
from jax.experimental.pallas import tpu as pltpu
from jax.sharding import PartitionSpec as P

norm_eps = 1e-06
SIDE = 2
PLANE = SIDE * SIDE
TURNED = 4
LINE = 4
MESH = pl.DeviceIdType.MESH


def shards(resid_stream, pre_gain, w_gate, w_up, w_down, post_gain):
    stream = resid_stream.astype(jnp.float32)
    local_norm = stream * lax.rsqrt(jnp.mean(stream * stream, axis=1, keepdims=True) + norm_eps)
    normed = (local_norm * pre_gain).astype(jnp.bfloat16)
    row_piece = lax.all_gather(normed, "tensor", axis=0, tiled=True)
    gate_out = jnp.dot(row_piece, w_gate, preferred_element_type=jnp.float32)
    up_out = jnp.dot(row_piece, w_up, preferred_element_type=jnp.float32)
    hidden = (jax.nn.gelu(gate_out, approximate=True) * up_out).astype(jnp.bfloat16)
    block_rows = lax.psum_scatter(
        jnp.dot(hidden, w_down, preferred_element_type=jnp.float32),
        "tensor",
        scatter_dimension=0,
        tiled=True,
    )
    row_factor = lax.rsqrt(jnp.mean(block_rows * block_rows, axis=1, keepdims=True) + norm_eps)
    post = (block_rows * row_factor * post_gain).astype(jnp.bfloat16)
    post = lax.optimization_barrier(post)
    return (stream + post.astype(jnp.float32)).astype(jnp.bfloat16)


def tile_of(size, most):
    return max(t for t in range(128, most + 1, 128) if size % t == 0)


def cut(d):
    lanes = d // 128
    most = 2 * (TURNED * lanes // 36) + lanes % 2
    return (lanes - most) // 2 * 128, most * 128


ARRIVALS = [
    *((name, q) for name in ("xa", "yb", "rest", "da", "db", "ra", "rb") for q in range(LINE)),
    *((name, j) for name in ("za", "zb", "zo", "zc", "sa", "sb", "sc") for j in range(LINE - 1)),
    ("spread", 0),
    ("share", 0),
]
BATCH = 32
SENDS = 8


def kernel(
    stream_hbm, pre_hbm, wg_hbm, wu_hbm, wd_hbm, post_hbm, out_ref,
    stream_ref, pre_ref, post_ref, w1, w2, gath, gu, hid, part, sendb, rda, rdb, rr, zr, zc, xyc,
    lsem, ssem, rsem,
):
    rows, d = stream_ref.shape
    ff = wg_hbm.shape[1]
    half, cw = cut(d)
    group = PLANE * rows
    A, B = halves = pl.ds(0, half), pl.ds(half, half)
    AB = pl.ds(0, 2 * half)
    C = pl.ds(2 * half, cw)

    me = lax.axis_index("tensor")
    x = lax.rem(me, SIDE)
    y = lax.rem(lax.div(me, SIDE), SIDE)
    z = lax.div(me, PLANE)
    sx = 1 - 2 * x
    sy = SIDE * (1 - 2 * y)
    xn, yn, dn = me + sx, me + sy, me + sx + sy
    flip = lax.div(z, LINE // 2)
    step = PLANE * (1 - 2 * flip)
    place = z + flip * (LINE - 1 - 2 * z)
    far, near = me + step, me - step

    barrier = pltpu.get_barrier_semaphore()
    for other in (xn, yn, dn, far):
        pl.semaphore_signal(barrier, inc=1, device_id={"tensor": other}, device_id_type=MESH)

    @pl.when(place == 1)
    def _():
        pl.semaphore_signal(barrier, inc=1, device_id={"tensor": near}, device_id_type=MESH)

    loads = [
        pltpu.make_async_copy(src, dst, lsem.at[i])
        for i, (src, dst) in enumerate(
            (
                (stream_hbm, stream_ref),
                (pre_hbm, pre_ref),
                (wg_hbm, w1.at[:, pl.ds(0, ff)]),
                (wu_hbm, w1.at[:, pl.ds(ff, ff)]),
                (wd_hbm, w2),
                (post_hbm, post_ref),
            )
        )
    ]
    for load in loads:
        load.start()
    loads[0].wait()
    loads[1].wait()

    def blk(q, r, n=1):
        return pl.ds((q * PLANE + r) * rows, n * rows)

    def normed():
        stream = stream_ref[...].astype(jnp.float32)
        scale = lax.rsqrt(jnp.mean(stream * stream, axis=1, keepdims=True) + norm_eps)
        return (stream * scale * pre_ref[...][None]).astype(jnp.bfloat16)

    def run(p):
        sent = []

        def send(src, dst, name, target):
            width = src.shape[-1]
            units = src.size // (rows * width) if hasattr(src, "size") else src.shape[0] // rows
            for slot, entry in enumerate(sent):
                if entry[0] == width and entry[1] + units <= BATCH:
                    entry[1] += units
                    break
            else:
                slot = len(sent)
                sent.append([width, units])
            pltpu.make_async_remote_copy(
                src_ref=src, dst_ref=dst, send_sem=ssem.at[slot], recv_sem=rsem.at[ARRIVALS.index(name)],
                device_id={"tensor": target}, device_id_type=MESH,
            ).start()

        def arrive(dst, *name):
            pltpu.make_async_remote_copy(
                src_ref=dst, dst_ref=dst, send_sem=ssem.at[0], recv_sem=rsem.at[ARRIVALS.index(name)],
                device_id={"tensor": xn}, device_id_type=MESH,
            ).wait_recv()

        def slot_of(q, owner):
            return [v for v in range(LINE) if v != owner].index(q)

        def along(at, cols, kind, q):
            ref = gath.at[at, cols]
            rel = at.start - q * group
            there = lambda v: gath.at[pl.ds(v * group + rel, at.size), cols]
            if p == 0:
                if q == 0:
                    send(ref, there(0), (kind, slot_of(0, 1)), far)
            else:
                if q in (0, 1):
                    send(ref, there(LINE - 1 - q), (kind, slot_of(LINE - 1 - q, 1)), far)
                if q in (1, 2, 3):
                    send(ref, there(q), (kind, slot_of(q, 0)), near)

        def zin(q, kind):
            at = blk(q, 1, 3) if kind == "zc" else blk(q, 0)
            cols = {"za": A, "zb": B}.get(kind, C)
            arrive(gath.at[at, cols], kind, slot_of(q, p))
            along(at, cols, kind, q)

        def first_a(q):
            send(gath.at[blk(q, 0), A], gath.at[blk(q, 1), A], ("xa", q), xn)

        def first_b(q):
            send(gath.at[blk(q, 0), B], gath.at[blk(q, 2), B], ("yb", q), yn)

        def second(q):
            send(gath.at[blk(q, 0), B], gath.at[blk(q, 1), B], ("rest", q), xn)
            send(gath.at[blk(q, 0), A], gath.at[blk(q, 2), A], ("rest", q), yn)

        def pass_a(q):
            zin(q, "za")
            first_a(q)

        def pass_b(q):
            zin(q, "zb")
            first_b(q)
            second(q)

        def relay(q):
            arrive(gath.at[blk(q, 1), A], "xa", q)
            send(gath.at[blk(q, 1), A], gath.at[blk(q, 3), A], ("rest", q), yn)
            arrive(gath.at[blk(q, 2), B], "yb", q)
            send(gath.at[blk(q, 2), B], gath.at[blk(q, 3), B], ("rest", q), xn)

        def start():
            own = gath.at[blk(p, 0), C]
            along(blk(p, 0), A, "za", p)
            first_a(p)
            along(blk(p, 0), B, "zb", p)
            first_b(p)
            along(blk(p, 0), C, "zo", p)
            for r, other in ((1, xn), (2, yn), (3, dn)):
                send(own, gath.at[blk(p, r), C], ("spread", 0), other)
            second(p)

        def spread():
            arrive(gath.at[blk(p, 1, 3), C], "spread", 0)
            along(blk(p, 1, 3), C, "zc", p)

        tile = tile_of(2 * ff, 256)
        wide = tile_of(d, 384)

        def full(q):
            arrive(gath.at[blk(q, 0, 4), A], "rest", q)

        def first(q, n=1):
            at = blk(q, 0, n * PLANE)
            up_to = pl.ds(0, n * group)

            @pl.loop(0, 2 * ff // tile)
            def _(i):
                cols = pl.ds(pl.multiple_of(i * tile, tile), tile)
                gu[up_to, cols] = jnp.dot(gath[at, :], w1[:, cols], preferred_element_type=jnp.float32)

            gate, up = gu[up_to, :ff], gu[up_to, ff:]
            hid[at, :] = (jax.nn.gelu(gate, approximate=True) * up).astype(jnp.bfloat16)

        def last(q, n=1):
            at = blk(q, 0, n * PLANE)

            @pl.loop(0, d // wide)
            def _(i):
                cols = pl.ds(pl.multiple_of(i * wide, wide), wide)
                res = jnp.dot(hid[at, :], w2[:, cols], preferred_element_type=jnp.float32)
                part[at, cols] = res
                sendb[at, cols] = res.astype(jnp.bfloat16)

        if p == 0:
            ways = {1: (far, 0), 2: (far, 1), 3: (me + 3 * step, 2)}
        else:
            ways = {0: (near, 0), 2: (far, 2), 3: (far + step, 1)}
        gather_slots = {0: (), 1: ()} if p == 0 else {0: (), 2: (1,), 3: ()}
        gather_slots[2] = (1,) if p == 1 else ()
        gather_slots[3] = ()
        gather_slots[p] = (0, 1, 2) if p == 0 else (0, 2)

        def turn(q):
            for slot in gather_slots[q]:
                arrive(zc.at[slot], "sc", slot)
                part[blk(q, 0, 4), C] += zc[slot].astype(jnp.float32)
            if gather_slots[q]:
                sendb[blk(q, 0, 4), C] = part[blk(q, 0, 4), C].astype(jnp.bfloat16)
            target, slot = ways[q]
            send(sendb.at[blk(q, 0, 4), C], zc.at[slot], ("sc", slot), target)

        def out_diag(q):
            send(sendb.at[blk(q, 3), A], rda.at[q], ("da", q), xn)
            send(sendb.at[blk(q, 3), B], rdb.at[q], ("db", q), yn)

        def out_side(q):
            send(sendb.at[blk(q, 1), A], rr.at[q, 0, :, A], ("ra", q), xn)
            send(sendb.at[blk(q, 2), B], rr.at[q, 1, :, B], ("rb", q), yn)

        def pass_on(q):
            arrive(rda.at[q], "da", q)
            at = blk(q, 2)
            sendb[at, A] = (part[at, A] + rda[q].astype(jnp.float32)).astype(jnp.bfloat16)
            send(sendb.at[at, A], rr.at[q, 1, :, A], ("ra", q), yn)
            arrive(rdb.at[q], "db", q)
            at = blk(q, 1)
            sendb[at, B] = (part[at, B] + rdb[q].astype(jnp.float32)).astype(jnp.bfloat16)
            send(sendb.at[at, B], rr.at[q, 0, :, B], ("rb", q), xn)

        def settle(q):
            at = blk(q, 0)
            for cols, name, sname in ((A, "ra", "sa"), (B, "rb", "sb")):
                arrive(rr.at[q, :, :, cols], name, q)
                total = part[at, cols] + rr[q, 0, :, cols].astype(jnp.float32) + rr[q, 1, :, cols].astype(jnp.float32)
                if q != p:
                    for slot in gather_slots[q]:
                        arrive(zr.at[slot, :, cols], sname, slot)
                        total += zr[slot, :, cols].astype(jnp.float32)
                    sendb[at, cols] = total.astype(jnp.bfloat16)
                    target, slot = ways[q]
                    send(sendb.at[at, cols], zr.at[slot, :, cols], (sname, slot), target)
                else:
                    part[at, cols] = total

        def share():
            for slot in gather_slots[p]:
                arrive(zc.at[slot], "sc", slot)
                part[blk(p, 0, 4), C] += zc[slot].astype(jnp.float32)
            sendb[blk(p, 1, 3), C] = part[blk(p, 1, 3), C].astype(jnp.bfloat16)
            for r, other in ((1, xn), (2, yn), (3, dn)):
                send(sendb.at[blk(p, r), C], xyc.at[pl.ds((r - 1) * rows, rows)], ("share", 0), other)

        def close():
            at = blk(p, 0)
            for slot in gather_slots[p]:
                for cols, sname in ((A, "sa"), (B, "sb")):
                    arrive(zr.at[slot, :, cols], sname, slot)
                    part[at, cols] += zr[slot, :, cols].astype(jnp.float32)

        def gain():
            arrive(xyc.at[...], "share", 0)
            more = xyc[...].astype(jnp.float32).reshape(3, rows, cw)
            part[blk(p, 0), C] += more[0] + more[1] + more[2]

        def finish():
            total = part[blk(p, 0), :]
            factor = lax.rsqrt(jnp.mean(total * total, axis=1, keepdims=True) + norm_eps)
            post = (total * factor * post_ref[...][None]).astype(jnp.bfloat16)
            stream = stream_ref[...].astype(jnp.float32)
            out_ref[...] = (stream + post.astype(jnp.float32)).astype(jnp.bfloat16)

        def drain():
            for slot, (width, units) in enumerate(sent):
                ref = part.at[pl.ds(0, units * rows // 2), pl.ds(0, width)]
                pltpu.make_async_remote_copy(
                    src_ref=ref, dst_ref=ref, send_sem=ssem.at[slot], recv_sem=rsem.at[0],
                    device_id={"tensor": xn}, device_id_type=MESH,
                ).wait_send()

        gath[blk(p, 0), :] = normed()
        pl.semaphore_wait(barrier, 4 + p)
        S = lambda f, *a: step_of(f, *a)
        if p == 0:
            S(start)
            S(pass_a, 1)
            S(pass_b, 1)
            S(spread)
            S(relay, 0)
            S(pass_a, 2)
            S(pass_b, 2)
            S(relay, 1)
            S(full, 0)
            loads[2].wait()
            loads[3].wait()
            S(first, 0)
            S(pass_a, 3)
            S(pass_b, 3)
            S(relay, 2)
            S(zin, 1, "zo")
            S(zin, 1, "zc")
            S(full, 1)
            S(first, 1)
            S(relay, 3)
            loads[4].wait()
            S(last, 0, 2)
            S(turn, 1)
            S(out_diag, 1)
            S(out_side, 1)
            S(zin, 2, "zo")
            S(zin, 2, "zc")
            S(full, 2)
            S(first, 2)
            S(pass_on, 1)
            S(zin, 3, "zo")
            S(zin, 3, "zc")
            S(full, 3)
            S(first, 3)
            S(last, 2, 2)
            S(turn, 3)
            S(out_diag, 3)
            S(out_diag, 2)
            S(out_side, 3)
            S(turn, 2)
            S(settle, 1)
            S(out_side, 2)
            S(pass_on, 3)
            S(pass_on, 2)
            S(out_diag, 0)
            S(out_side, 0)
            S(settle, 3)
            S(settle, 2)
            S(pass_on, 0)
            loads[5].wait()
            S(share)
            S(settle, 0)
            S(close)
            S(gain)
        else:
            S(start)
            S(pass_a, 0)
            S(pass_a, 2)
            S(pass_b, 0)
            S(pass_b, 2)
            S(zin, 0, "zo")
            S(zin, 2, "zo")
            S(relay, 1)
            S(spread)
            S(pass_a, 3)
            S(pass_b, 3)
            S(zin, 3, "zo")
            S(full, 1)
            loads[2].wait()
            loads[3].wait()
            S(first, 1)
            S(relay, 0)
            S(zin, 0, "zc")
            S(zin, 2, "zc")
            S(relay, 2)
            S(full, 0)
            S(first, 0)
            S(zin, 3, "zc")
            S(relay, 3)
            loads[4].wait()
            S(last, 0, 2)
            S(turn, 0)
            S(out_diag, 0)
            S(out_side, 0)
            S(full, 2)
            S(first, 2)
            S(pass_on, 0)
            S(full, 3)
            S(first, 3)
            S(last, 2, 2)
            S(turn, 3)
            S(out_diag, 3)
            S(out_diag, 2)
            S(out_side, 3)
            S(settle, 0)
            S(out_side, 2)
            S(pass_on, 3)
            S(turn, 2)
            S(pass_on, 2)
            S(out_diag, 1)
            S(out_side, 1)
            S(settle, 3)
            S(settle, 2)
            S(pass_on, 1)
            loads[5].wait()
            S(share)
            S(settle, 1)
            S(close)
            S(gain)
        S(finish)
        S(drain)

    for p in (0, 1):
        pl.when(place == p)(functools.partial(run, p))


def step_of(f, *args):
    with jax.named_scope(f.__name__ + "#" + "_".join(str(a) for a in args)):
        f(*args)


def fused(resid_stream, pre_gain, w_gate, w_up, w_down, post_gain):
    rows, d = resid_stream.shape
    ff = w_gate.shape[1]
    half, cw = cut(d)
    n = PLANE * LINE
    bf, f32, dma = jnp.bfloat16, jnp.float32, pltpu.SemaphoreType.DMA
    hbm = pl.BlockSpec(memory_space=pl.ANY)
    return pl.pallas_call(
        kernel,
        out_shape=pltpu.VMEM((rows, d), bf),
        in_specs=[hbm] * 6,
        out_specs=pl.BlockSpec(memory_space=pltpu.VMEM),
        scratch_shapes=[
            pltpu.VMEM((rows, d), bf),
            pltpu.VMEM((d,), f32),
            pltpu.VMEM((d,), f32),
            pltpu.VMEM((d, 2 * ff), bf),
            pltpu.VMEM((ff, d), bf),
            pltpu.VMEM((n * rows, d), bf),
            pltpu.VMEM((2 * PLANE * rows, 2 * ff), f32),
            pltpu.VMEM((n * rows, ff), bf),
            pltpu.VMEM((n * rows, d), f32),
            pltpu.VMEM((n * rows, d), bf),
            pltpu.VMEM((LINE, rows, half), bf),
            pltpu.VMEM((LINE, rows, half), bf),
            pltpu.VMEM((LINE, 2, rows, d), bf),
            pltpu.VMEM((LINE - 1, rows, 2 * half), bf),
            pltpu.VMEM((LINE - 1, PLANE * rows, cw), bf),
            pltpu.VMEM((3 * rows, cw), bf),
            dma((6,)),
            dma((SENDS,)),
            dma((len(ARRIVALS),)),
        ],
        compiler_params=pltpu.CompilerParams(
            collective_id=0, has_side_effects=True, vmem_limit_bytes=60 * 2**20
        ),
        name="ffn",
    )(resid_stream, pre_gain, w_gate, w_up, w_down, post_gain)


def solution(mesh):
    body = fused if mesh.shape["tensor"] == PLANE * LINE else shards
    return jax.shard_map(
        body,
        mesh=mesh,
        in_specs=(
            P(("dp", "tensor"), None),
            P(),
            P(None, "tensor"),
            P(None, "tensor"),
            P("tensor", None),
            P(),
        ),
        out_specs=P(("dp", "tensor"), None),
        check_vma=False,
    )
```

```python
import functools

import jax
import jax.numpy as jnp
from jax import lax
from jax.experimental import pallas as pl
from jax.experimental.pallas import tpu as pltpu
from jax.sharding import PartitionSpec as P

norm_eps = 1e-06
SIDE = 2
PLANE = SIDE * SIDE
TURNED = 4
LINE = 4
MESH = pl.DeviceIdType.MESH


def shards(resid_stream, pre_gain, w_gate, w_up, w_down, post_gain):
    stream = resid_stream.astype(jnp.float32)
    local_norm = stream * lax.rsqrt(jnp.mean(stream * stream, axis=1, keepdims=True) + norm_eps)
    normed = (local_norm * pre_gain).astype(jnp.bfloat16)
    row_piece = lax.all_gather(normed, "tensor", axis=0, tiled=True)
    gate_out = jnp.dot(row_piece, w_gate, preferred_element_type=jnp.float32)
    up_out = jnp.dot(row_piece, w_up, preferred_element_type=jnp.float32)
    hidden = (jax.nn.gelu(gate_out, approximate=True) * up_out).astype(jnp.bfloat16)
    block_rows = lax.psum_scatter(
        jnp.dot(hidden, w_down, preferred_element_type=jnp.float32),
        "tensor",
        scatter_dimension=0,
        tiled=True,
    )
    row_factor = lax.rsqrt(jnp.mean(block_rows * block_rows, axis=1, keepdims=True) + norm_eps)
    post = (block_rows * row_factor * post_gain).astype(jnp.bfloat16)
    post = lax.optimization_barrier(post)
    return (stream + post.astype(jnp.float32)).astype(jnp.bfloat16)


def tile_of(size, most):
    return max(t for t in range(128, most + 1, 128) if size % t == 0)


def cut(d):
    lanes = d // 128
    most = 2 * (TURNED * lanes // 36) + lanes % 2
    return (lanes - most) // 2 * 128, most * 128


ARRIVALS = [
    *((name, q) for name in ("xa", "yb", "rest", "da", "db", "ra", "rb") for q in range(LINE)),
    *((name, j) for name in ("za", "zb", "zo", "zc", "sa", "sb", "sc") for j in range(LINE - 1)),
    ("spread", 0),
    ("share", 0),
]
BATCH = 32
SENDS = 8

PROGRAMS = (
    (
        ("start",), ("relay_a", 0), ("pass_a", 1), ("pass_b", 1), ("zo", 1), ("relay_b", 0), ("spread",),
        ("pass_a", 2), ("relay_a", 1), ("pass_b", 2), ("relay_b", 1), ("zo", 2), ("first", 0), ("zc_", 1),
        ("relay_a", 2), ("pass_a", 3), ("relay_b", 2), ("pass_b", 3), ("first", 1), ("zo", 3), ("relay_a", 3),
        ("last", 1), ("zc_", 2), ("relay_b", 3), ("turn", 1), ("out_side", 1), ("out_diag", 1), ("first", 2),
        ("last", 2), ("zc_", 3), ("turn", 2), ("out_diag", 2), ("out_side", 2), ("first", 3), ("pass_on_b", 1),
        ("last", 3), ("out_diag", 3), ("turn", 3), ("pass_on_a", 1), ("pass_on_b", 2), ("pass_on_a", 2),
        ("settle_b", 1), ("pass_on_b", 3), ("pass_on_a", 3), ("out_side", 3), ("settle_a", 1), ("settle_b", 2),
        ("settle_a", 2), ("last", 0), ("out_diag", 0), ("share",), ("out_side", 0), ("settle_a", 3), ("settle_b", 3),
        ("pass_on_a", 0), ("pass_on_b", 0), ("gain",), ("settle_a", 0), ("settle_b", 0), ("close",), ("finish",),
        ("drain",),
    ),
    (
        ("start",), ("pass_a", 0), ("pass_a", 2), ("pass_b", 0), ("pass_b", 2), ("zo", 0), ("zo", 2), ("spread",),
        ("pass_a", 3), ("relay_a", 0), ("pass_b", 3), ("relay_b", 0), ("zo", 3), ("zc_", 0), ("relay_a", 1),
        ("relay_b", 2), ("zc_", 2), ("relay_a", 3), ("relay_b", 3), ("relay_b", 1), ("zc_", 3), ("first", 0),
        ("relay_a", 2), ("last", 0), ("turn", 0), ("out_diag", 0), ("out_side", 0), ("first", 3), ("last", 3),
        ("turn", 3), ("out_diag", 3), ("out_side", 3), ("first", 2), ("pass_on_b", 0), ("pass_on_a", 0), ("last", 2),
        ("out_diag", 2), ("first", 1), ("pass_on_a", 3), ("pass_on_b", 3), ("turn", 2), ("last", 1), ("settle_b", 0),
        ("settle_a", 0), ("out_side", 1), ("out_diag", 1), ("out_side", 2), ("pass_on_a", 2), ("pass_on_b", 2),
        ("settle_a", 3), ("settle_b", 3), ("share",), ("pass_on_a", 1), ("pass_on_b", 1), ("settle_a", 2),
        ("settle_b", 2), ("settle_a", 1), ("settle_b", 1), ("gain",), ("close",), ("finish",), ("drain",),
    ),
)


def kernel(
    stream_hbm, pre_hbm, wg_hbm, wu_hbm, wd_hbm, post_hbm, out_ref,
    stream_ref, pre_ref, post_ref, w1, w2, gath, gu, hid, part, sendb, rda, rdb, rr, zr, zc, xyc,
    lsem, ssem, rsem,
):
    rows, d = stream_ref.shape
    ff = wg_hbm.shape[1]
    half, cw = cut(d)
    group = PLANE * rows
    A, B = halves = pl.ds(0, half), pl.ds(half, half)
    AB = pl.ds(0, 2 * half)
    C = pl.ds(2 * half, cw)

    me = lax.axis_index("tensor")
    x = lax.rem(me, SIDE)
    y = lax.rem(lax.div(me, SIDE), SIDE)
    z = lax.div(me, PLANE)
    sx = 1 - 2 * x
    sy = SIDE * (1 - 2 * y)
    xn, yn, dn = me + sx, me + sy, me + sx + sy
    flip = lax.div(z, LINE // 2)
    step = PLANE * (1 - 2 * flip)
    place = z + flip * (LINE - 1 - 2 * z)
    far, near = me + step, me - step

    barrier = pltpu.get_barrier_semaphore()
    for other in (xn, yn, dn, far):
        pl.semaphore_signal(barrier, inc=1, device_id={"tensor": other}, device_id_type=MESH)

    @pl.when(place == 1)
    def _():
        pl.semaphore_signal(barrier, inc=1, device_id={"tensor": near}, device_id_type=MESH)

    loads = [
        pltpu.make_async_copy(src, dst, lsem.at[i])
        for i, (src, dst) in enumerate(
            (
                (stream_hbm, stream_ref),
                (pre_hbm, pre_ref),
                (wg_hbm, w1.at[:, pl.ds(0, ff)]),
                (wu_hbm, w1.at[:, pl.ds(ff, ff)]),
                (wd_hbm, w2),
                (post_hbm, post_ref),
            )
        )
    ]
    for load in loads:
        load.start()
    loads[0].wait()
    loads[1].wait()

    def blk(q, r, n=1):
        return pl.ds((q * PLANE + r) * rows, n * rows)

    def normed():
        stream = stream_ref[...].astype(jnp.float32)
        scale = lax.rsqrt(jnp.mean(stream * stream, axis=1, keepdims=True) + norm_eps)
        return (stream * scale * pre_ref[...][None]).astype(jnp.bfloat16)

    def run(p):
        sent = []
        loaded = set()

        def send(src, dst, name, target):
            width = src.shape[-1]
            units = src.size // (rows * width) if hasattr(src, "size") else src.shape[0] // rows
            for slot, entry in enumerate(sent):
                if entry[0] == width and entry[1] + units <= BATCH:
                    entry[1] += units
                    break
            else:
                slot = len(sent)
                sent.append([width, units])
            pltpu.make_async_remote_copy(
                src_ref=src, dst_ref=dst, send_sem=ssem.at[slot], recv_sem=rsem.at[ARRIVALS.index(name)],
                device_id={"tensor": target}, device_id_type=MESH,
            ).start()

        def arrive(dst, *name):
            pltpu.make_async_remote_copy(
                src_ref=dst, dst_ref=dst, send_sem=ssem.at[0], recv_sem=rsem.at[ARRIVALS.index(name)],
                device_id={"tensor": xn}, device_id_type=MESH,
            ).wait_recv()

        def slot_of(q, owner):
            return [v for v in range(LINE) if v != owner].index(q)

        def along(at, cols, kind, q):
            ref = gath.at[at, cols]
            rel = at.start - q * group
            there = lambda v: gath.at[pl.ds(v * group + rel, at.size), cols]
            if p == 0:
                if q == 0:
                    send(ref, there(0), (kind, slot_of(0, 1)), far)
            else:
                if q in (0, 1):
                    send(ref, there(LINE - 1 - q), (kind, slot_of(LINE - 1 - q, 1)), far)
                if q in (1, 2, 3):
                    send(ref, there(q), (kind, slot_of(q, 0)), near)

        def zo(q):
            zin(q, "zo")

        def zc_(q):
            zin(q, "zc")

        def zin(q, kind):
            at = blk(q, 1, 3) if kind == "zc" else blk(q, 0)
            cols = {"za": A, "zb": B}.get(kind, C)
            arrive(gath.at[at, cols], kind, slot_of(q, p))
            along(at, cols, kind, q)

        def first_a(q):
            send(gath.at[blk(q, 0), A], gath.at[blk(q, 1), A], ("xa", q), xn)

        def first_b(q):
            send(gath.at[blk(q, 0), B], gath.at[blk(q, 2), B], ("yb", q), yn)

        def second(q):
            send(gath.at[blk(q, 0), B], gath.at[blk(q, 1), B], ("rest", q), xn)
            send(gath.at[blk(q, 0), A], gath.at[blk(q, 2), A], ("rest", q), yn)

        def pass_a(q):
            zin(q, "za")
            first_a(q)

        def pass_b(q):
            zin(q, "zb")
            first_b(q)
            second(q)

        def relay_a(q):
            arrive(gath.at[blk(q, 1), A], "xa", q)
            send(gath.at[blk(q, 1), A], gath.at[blk(q, 3), A], ("rest", q), yn)

        def relay_b(q):
            arrive(gath.at[blk(q, 2), B], "yb", q)
            send(gath.at[blk(q, 2), B], gath.at[blk(q, 3), B], ("rest", q), xn)

        def start():
            own = gath.at[blk(p, 0), C]
            along(blk(p, 0), A, "za", p)
            first_a(p)
            along(blk(p, 0), B, "zb", p)
            first_b(p)
            along(blk(p, 0), C, "zo", p)
            for r, other in ((1, xn), (2, yn), (3, dn)):
                send(own, gath.at[blk(p, r), C], ("spread", 0), other)
            second(p)

        def spread():
            arrive(gath.at[blk(p, 1, 3), C], "spread", 0)
            along(blk(p, 1, 3), C, "zc", p)

        tile = tile_of(2 * ff, 256)
        wide = tile_of(d, 768)

        def full(q):
            arrive(gath.at[blk(q, 0, 4), A], "rest", q)

        def first(q, n=1):
            for v in range(q, q + n):
                full(v)
            if "in" not in loaded:
                loaded.add("in")
                loads[2].wait()
                loads[3].wait()
            at = blk(q, 0, n * PLANE)
            up_to = pl.ds(0, n * group)

            @pl.loop(0, 2 * ff // tile)
            def _(i):
                cols = pl.ds(pl.multiple_of(i * tile, tile), tile)
                gu[up_to, cols] = jnp.dot(gath[at, :], w1[:, cols], preferred_element_type=jnp.float32)

            gate, up = gu[up_to, :ff], gu[up_to, ff:]
            hid[at, :] = (jax.nn.gelu(gate, approximate=True) * up).astype(jnp.bfloat16)

        def last(q, n=1):
            if "out" not in loaded:
                loaded.add("out")
                loads[4].wait()
            at = blk(q, 0, n * PLANE)

            @pl.loop(0, d // wide)
            def _(i):
                cols = pl.ds(pl.multiple_of(i * wide, wide), wide)
                res = jnp.dot(hid[at, :], w2[:, cols], preferred_element_type=jnp.float32)
                part[at, cols] = res
                sendb[at, cols] = res.astype(jnp.bfloat16)

        if p == 0:
            ways = {1: (far, 0), 2: (far, 1), 3: (me + 3 * step, 2)}
        else:
            ways = {0: (near, 0), 2: (far, 2), 3: (far + step, 1)}
        gather_slots = {0: (), 1: ()} if p == 0 else {0: (), 2: (1,), 3: ()}
        gather_slots[2] = (1,) if p == 1 else ()
        gather_slots[3] = ()
        gather_slots[p] = (0, 1, 2) if p == 0 else (0, 2)

        def turn(q):
            for slot in gather_slots[q]:
                arrive(zc.at[slot], "sc", slot)
                part[blk(q, 0, 4), C] += zc[slot].astype(jnp.float32)
            if gather_slots[q]:
                sendb[blk(q, 0, 4), C] = part[blk(q, 0, 4), C].astype(jnp.bfloat16)
            target, slot = ways[q]
            send(sendb.at[blk(q, 0, 4), C], zc.at[slot], ("sc", slot), target)

        def out_diag(q):
            send(sendb.at[blk(q, 3), A], rda.at[q], ("da", q), xn)
            send(sendb.at[blk(q, 3), B], rdb.at[q], ("db", q), yn)

        def out_side(q):
            send(sendb.at[blk(q, 1), A], rr.at[q, 0, :, A], ("ra", q), xn)
            send(sendb.at[blk(q, 2), B], rr.at[q, 1, :, B], ("rb", q), yn)

        def pass_on_a(q):
            arrive(rda.at[q], "da", q)
            at = blk(q, 2)
            sendb[at, A] = (part[at, A] + rda[q].astype(jnp.float32)).astype(jnp.bfloat16)
            send(sendb.at[at, A], rr.at[q, 1, :, A], ("ra", q), yn)

        def pass_on_b(q):
            arrive(rdb.at[q], "db", q)
            at = blk(q, 1)
            sendb[at, B] = (part[at, B] + rdb[q].astype(jnp.float32)).astype(jnp.bfloat16)
            send(sendb.at[at, B], rr.at[q, 0, :, B], ("rb", q), xn)

        def settle(q, cols, name, sname):
            at = blk(q, 0)
            arrive(rr.at[q, :, :, cols], name, q)
            total = part[at, cols] + rr[q, 0, :, cols].astype(jnp.float32) + rr[q, 1, :, cols].astype(jnp.float32)
            if q == p:
                part[at, cols] = total
                return
            for slot in gather_slots[q]:
                arrive(zr.at[slot, :, cols], sname, slot)
                total += zr[slot, :, cols].astype(jnp.float32)
            sendb[at, cols] = total.astype(jnp.bfloat16)
            target, slot = ways[q]
            send(sendb.at[at, cols], zr.at[slot, :, cols], (sname, slot), target)

        def settle_a(q):
            settle(q, A, "ra", "sa")

        def settle_b(q):
            settle(q, B, "rb", "sb")

        def share():
            for slot in gather_slots[p]:
                arrive(zc.at[slot], "sc", slot)
                part[blk(p, 0, 4), C] += zc[slot].astype(jnp.float32)
            sendb[blk(p, 1, 3), C] = part[blk(p, 1, 3), C].astype(jnp.bfloat16)
            for r, other in ((1, xn), (2, yn), (3, dn)):
                send(sendb.at[blk(p, r), C], xyc.at[pl.ds((r - 1) * rows, rows)], ("share", 0), other)

        def close():
            at = blk(p, 0)
            for slot in gather_slots[p]:
                for cols, sname in ((A, "sa"), (B, "sb")):
                    arrive(zr.at[slot, :, cols], sname, slot)
                    part[at, cols] += zr[slot, :, cols].astype(jnp.float32)

        def gain():
            arrive(xyc.at[...], "share", 0)
            more = xyc[...].astype(jnp.float32).reshape(3, rows, cw)
            part[blk(p, 0), C] += more[0] + more[1] + more[2]

        def finish():
            loads[5].wait()
            total = part[blk(p, 0), :]
            factor = lax.rsqrt(jnp.mean(total * total, axis=1, keepdims=True) + norm_eps)
            post = (total * factor * post_ref[...][None]).astype(jnp.bfloat16)
            stream = stream_ref[...].astype(jnp.float32)
            out_ref[...] = (stream + post.astype(jnp.float32)).astype(jnp.bfloat16)

        def drain():
            for slot, (width, units) in enumerate(sent):
                ref = part.at[pl.ds(0, units * rows // 2), pl.ds(0, width)]
                pltpu.make_async_remote_copy(
                    src_ref=ref, dst_ref=ref, send_sem=ssem.at[slot], recv_sem=rsem.at[0],
                    device_id={"tensor": xn}, device_id_type=MESH,
                ).wait_send()

        gath[blk(p, 0), :] = normed()
        pl.semaphore_wait(barrier, 4 + p)
        steps = {f.__name__: f for f in (
            start, spread, share, close, gain, finish, drain, pass_a, pass_b, zo, zc_, relay_a, relay_b, first, last,
            turn, out_diag, out_side, pass_on_a, pass_on_b, settle_a, settle_b,
        )}
        for name, *args in PROGRAMS[p]:
            step_of(steps[name], *args)

    for p in (0, 1):
        pl.when(place == p)(functools.partial(run, p))


def step_of(f, *args):
    with jax.named_scope(f.__name__ + "#" + "_".join(str(a) for a in args)):
        f(*args)


def fused(resid_stream, pre_gain, w_gate, w_up, w_down, post_gain):
    rows, d = resid_stream.shape
    ff = w_gate.shape[1]
    half, cw = cut(d)
    n = PLANE * LINE
    bf, f32, dma = jnp.bfloat16, jnp.float32, pltpu.SemaphoreType.DMA
    hbm = pl.BlockSpec(memory_space=pl.ANY)
    return pl.pallas_call(
        kernel,
        out_shape=pltpu.VMEM((rows, d), bf),
        in_specs=[hbm] * 6,
        out_specs=pl.BlockSpec(memory_space=pltpu.VMEM),
        scratch_shapes=[
            pltpu.VMEM((rows, d), bf),
            pltpu.VMEM((d,), f32),
            pltpu.VMEM((d,), f32),
            pltpu.VMEM((d, 2 * ff), bf),
            pltpu.VMEM((ff, d), bf),
            pltpu.VMEM((n * rows, d), bf),
            pltpu.VMEM((2 * PLANE * rows, 2 * ff), f32),
            pltpu.VMEM((n * rows, ff), bf),
            pltpu.VMEM((n * rows, d), f32),
            pltpu.VMEM((n * rows, d), bf),
            pltpu.VMEM((LINE, rows, half), bf),
            pltpu.VMEM((LINE, rows, half), bf),
            pltpu.VMEM((LINE, 2, rows, d), bf),
            pltpu.VMEM((LINE - 1, rows, 2 * half), bf),
            pltpu.VMEM((LINE - 1, PLANE * rows, cw), bf),
            pltpu.VMEM((3 * rows, cw), bf),
            dma((6,)),
            dma((SENDS,)),
            dma((len(ARRIVALS),)),
        ],
        compiler_params=pltpu.CompilerParams(
            collective_id=0, has_side_effects=True, vmem_limit_bytes=60 * 2**20
        ),
        name="ffn",
    )(resid_stream, pre_gain, w_gate, w_up, w_down, post_gain)


def solution(mesh):
    body = fused if mesh.shape["tensor"] == PLANE * LINE else shards
    return jax.shard_map(
        body,
        mesh=mesh,
        in_specs=(
            P(("dp", "tensor"), None),
            P(),
            P(None, "tensor"),
            P(None, "tensor"),
            P("tensor", None),
            P(),
        ),
        out_specs=P(("dp", "tensor"), None),
        check_vma=False,
    )
```

```python
import functools

import jax
import jax.numpy as jnp
from jax import lax
from jax.experimental import pallas as pl
from jax.experimental.pallas import tpu as pltpu
from jax.sharding import PartitionSpec as P

norm_eps = 1e-06
SIDE = 2
PLANE = SIDE * SIDE
OUT_END, OUT_MID, BACK_END, BACK_MID = 7, 3, 4, 4
LINE = 4
MESH = pl.DeviceIdType.MESH


def shards(resid_stream, pre_gain, w_gate, w_up, w_down, post_gain):
    stream = resid_stream.astype(jnp.float32)
    local_norm = stream * lax.rsqrt(jnp.mean(stream * stream, axis=1, keepdims=True) + norm_eps)
    normed = (local_norm * pre_gain).astype(jnp.bfloat16)
    row_piece = lax.all_gather(normed, "tensor", axis=0, tiled=True)
    gate_out = jnp.dot(row_piece, w_gate, preferred_element_type=jnp.float32)
    up_out = jnp.dot(row_piece, w_up, preferred_element_type=jnp.float32)
    hidden = (jax.nn.gelu(gate_out, approximate=True) * up_out).astype(jnp.bfloat16)
    block_rows = lax.psum_scatter(
        jnp.dot(hidden, w_down, preferred_element_type=jnp.float32),
        "tensor",
        scatter_dimension=0,
        tiled=True,
    )
    row_factor = lax.rsqrt(jnp.mean(block_rows * block_rows, axis=1, keepdims=True) + norm_eps)
    post = (block_rows * row_factor * post_gain).astype(jnp.bfloat16)
    post = lax.optimization_barrier(post)
    return (stream + post.astype(jnp.float32)).astype(jnp.bfloat16)


def cut(d, turned):
    lanes = d // 128
    most = 2 * (turned * lanes // 36) + lanes % 2
    return (lanes - most) // 2 * 128, most * 128


def parts(d, turned):
    half, cw = cut(d, turned)
    return pl.ds(0, half), pl.ds(half, half), pl.ds(2 * half, cw)


BATCH = 32
WAYS = 5
E3_AB, E3_C, I3_AB, I3_C = True, True, True, True
KIND = ("zo", "z1", "z2", "z3")
ARRIVALS = [
    *((name, q) for name in ("xa", "yb", "rest", "da", "db", "ra", "rb") for q in range(LINE)),
    *((name, j) for name in ("za", "zb", "zo", "z1", "z2", "z3") for j in range(LINE - 1)),
    *((name, i) for name in ("sa", "sb", "sc") for i in range(WAYS)),
    *(("spread", r) for r in range(1, PLANE)),
    ("share", 0),
]
SENDS = 12


def kernel(
    stream_hbm, pre_hbm, wg_hbm, wu_hbm, wd_hbm, post_hbm, out_ref,
    stream_ref, pre_ref, post_ref, w1, w2, gath, gu, hid, part, sendb, rd, rr, zr, zrc, xyc,
    lsem, ssem, rsem,
):
    rows, d = stream_ref.shape
    ff = wg_hbm.shape[1]
    group = PLANE * rows
    out_cols, back_cols = ([parts(d, v) for v in (e, m, m, e)] for e, m in ((OUT_END, OUT_MID), (BACK_END, BACK_MID)))

    me = lax.axis_index("tensor")
    x = lax.rem(me, SIDE)
    y = lax.rem(lax.div(me, SIDE), SIDE)
    z = lax.div(me, PLANE)
    sx = 1 - 2 * x
    sy = SIDE * (1 - 2 * y)
    xn, yn, dn = me + sx, me + sy, me + sx + sy
    flip = lax.div(z, LINE // 2)
    step = PLANE * (1 - 2 * flip)
    place = z + flip * (LINE - 1 - 2 * z)
    far, near = me + step, me - step

    barrier = pltpu.get_barrier_semaphore()
    for other in (xn, yn, dn, far):
        pl.semaphore_signal(barrier, inc=1, device_id={"tensor": other}, device_id_type=MESH)

    @pl.when(place == 1)
    def _():
        pl.semaphore_signal(barrier, inc=1, device_id={"tensor": near}, device_id_type=MESH)

    loads = [
        pltpu.make_async_copy(src, dst, lsem.at[i])
        for i, (src, dst) in enumerate(
            (
                (stream_hbm, stream_ref),
                (pre_hbm, pre_ref),
                (wg_hbm, w1.at[:, pl.ds(0, ff)]),
                (wu_hbm, w1.at[:, pl.ds(ff, ff)]),
                (wd_hbm, w2),
                (post_hbm, post_ref),
            )
        )
    ]
    for load in loads:
        load.start()
    loads[0].wait()
    loads[1].wait()

    def blk(q, r, n=1):
        return pl.ds((q * PLANE + r) * rows, n * rows)

    def normed():
        stream = stream_ref[...].astype(jnp.float32)
        scale = lax.rsqrt(jnp.mean(stream * stream, axis=1, keepdims=True) + norm_eps)
        return (stream * scale * pre_ref[...][None]).astype(jnp.bfloat16)

    def run(v):
        p = min(v, LINE - 1 - v)
        sent = []
        loaded, gated = set(), set()

        def send(src, dst, name, target):
            width = src.shape[-1]
            units = src.size // (rows * width) if hasattr(src, "size") else src.shape[0] // rows
            for slot, entry in enumerate(sent):
                if entry[0] == width and entry[1] + units <= BATCH:
                    entry[1] += units
                    break
            else:
                slot = len(sent)
                sent.append([width, units])
            pltpu.make_async_remote_copy(
                src_ref=src, dst_ref=dst, send_sem=ssem.at[slot], recv_sem=rsem.at[ARRIVALS.index(name)],
                device_id={"tensor": target}, device_id_type=MESH,
            ).start()

        def arrive(dst, *name):
            pltpu.make_async_remote_copy(
                src_ref=dst, dst_ref=dst, send_sem=ssem.at[0], recv_sem=rsem.at[ARRIVALS.index(name)],
                device_id={"tensor": xn}, device_id_type=MESH,
            ).wait_recv()

        def slot_of(q, owner):
            return [v for v in range(LINE) if v != owner].index(q)

        def along(at, cols, kind, q):
            ref = gath.at[at, cols]
            rel = at.start - q * group
            there = lambda v: gath.at[pl.ds(v * group + rel, at.size), cols]
            if p == 0:
                if q == 0:
                    send(ref, there(0), (kind, slot_of(0, 1)), far)
            else:
                if q in (0, 1):
                    send(ref, there(LINE - 1 - q), (kind, slot_of(LINE - 1 - q, 1)), far)
                if q in (1, 2, 3):
                    send(ref, there(q), (kind, slot_of(q, 0)), near)

        def zo(q):
            zin(q, "zo")

        def zc(q, r):
            zin(q, KIND[r])

        def zin(q, kind):
            at = blk(q, int(kind[1])) if kind[1].isdigit() else blk(q, 0)
            cols = out_cols[q][{"za": 0, "zb": 1}.get(kind, 2)]
            arrive(gath.at[at, cols], kind, slot_of(q, p))
            along(at, cols, kind, q)

        def first_a(q):
            A = out_cols[q][0]
            send(gath.at[blk(q, 0), A], gath.at[blk(q, 1), A], ("xa", q), xn)

        def first_b(q):
            B = out_cols[q][1]
            send(gath.at[blk(q, 0), B], gath.at[blk(q, 2), B], ("yb", q), yn)

        def second(q):
            A, B, _ = out_cols[q]
            send(gath.at[blk(q, 0), B], gath.at[blk(q, 1), B], ("rest", q), xn)
            send(gath.at[blk(q, 0), A], gath.at[blk(q, 2), A], ("rest", q), yn)

        def pass_a(q):
            zin(q, "za")
            first_a(q)

        def pass_b(q):
            zin(q, "zb")
            first_b(q)
            second(q)

        def relay_a(q):
            A = out_cols[q][0]
            arrive(gath.at[blk(q, 1), A], "xa", q)
            send(gath.at[blk(q, 1), A], gath.at[blk(q, 3), A], ("rest", q), yn)

        def relay_b(q):
            B = out_cols[q][1]
            arrive(gath.at[blk(q, 2), B], "yb", q)
            send(gath.at[blk(q, 2), B], gath.at[blk(q, 3), B], ("rest", q), xn)

        def start():
            A, B, C = out_cols[p]
            own = gath.at[blk(p, 0), C]
            along(blk(p, 0), A, "za", p)
            first_a(p)
            along(blk(p, 0), B, "zb", p)
            first_b(p)
            along(blk(p, 0), C, "zo", p)
            for r, other in ((1, xn), (2, yn), (3, dn)):
                send(own, gath.at[blk(p, r), C], ("spread", r), other)
            second(p)

        def spread(r):
            C = out_cols[p][2]
            arrive(gath.at[blk(p, r), C], "spread", r)
            along(blk(p, r), C, KIND[r], p)

        def full(q):
            arrive(gath.at[blk(q, 0, 4), out_cols[q][0]], "rest", q)

        def first(q, n=1):
            for v in range(q, q + n):
                full(v)
            if "in" not in loaded:
                loaded.add("in")
                loads[2].wait()
                loads[3].wait()
            beside = [v for v in (q - 1, q + 1) if n == 1 and v in gated]
            low, m = (min(q, beside[0]), 2) if beside else (q, n)
            gated.update(range(q, q + n))
            gu[blk(0, 0, m * PLANE), :] = jnp.dot(
                gath[blk(low, 0, m * PLANE), :], w1[...], preferred_element_type=jnp.float32
            )
            own = blk(q - low, 0, n * PLANE)
            gate, up = gu[own, :ff], gu[own, ff:]
            hid[blk(q, 0, n * PLANE), :] = (jax.nn.gelu(gate, approximate=True) * up).astype(jnp.bfloat16)

        def last(q, n=1):
            if "out" not in loaded:
                loaded.add("out")
                loads[4].wait()
            at = blk(q, 0, n * PLANE)

            res = jnp.dot(hid[at, :], w2[...], preferred_element_type=jnp.float32)
            part[at, :] = res
            sendb[at, :] = res.astype(jnp.bfloat16)

        def way(q, end_direct, inner_direct):
            if p == 0:
                return {1: (far, 0), 2: (far, 1), 3: (me + 3 * step, 2) if end_direct else (far, 3)}[q]
            return {0: (near, 0), 2: (far, 2), 3: (far + step, 1) if inner_direct else (far, 4)}[q]

        def added(q, end_direct, inner_direct):
            if q == p:
                return (0, 2) if p else (0, *((1,) if inner_direct else ()), *((2,) if end_direct else ()))
            if p == 0:
                return ()
            return {0: () if inner_direct else (4,), 2: (1,), 3: () if end_direct else (3,)}[q]

        def line_sum(q, at, cols):
            for slot in added(q, E3_C, I3_C):
                arrive(zrc.at[slot, :, pl.ds(0, cols.size)], "sc", slot)
                part[at, cols] += zrc[slot, :, :cols.size].astype(jnp.float32)

        def turn(q):
            at, C = blk(q, 0, 4), back_cols[q][2]
            line_sum(q, at, C)
            if added(q, E3_C, I3_C):
                sendb[at, C] = part[at, C].astype(jnp.bfloat16)
            target, slot = way(q, E3_C, I3_C)
            send(sendb.at[at, C], zrc.at[slot, :, pl.ds(0, C.size)], ("sc", slot), target)

        def out_diag(q):
            A, B, _ = back_cols[q]
            send(sendb.at[blk(q, 3), A], rd.at[q, :, A], ("da", q), xn)
            send(sendb.at[blk(q, 3), B], rd.at[q, :, B], ("db", q), yn)

        def out_side(q):
            A, B, _ = back_cols[q]
            send(sendb.at[blk(q, 1), A], rr.at[q, 0, :, A], ("ra", q), xn)
            send(sendb.at[blk(q, 2), B], rr.at[q, 1, :, B], ("rb", q), yn)

        def pass_on_a(q):
            at, A = blk(q, 2), back_cols[q][0]
            arrive(rd.at[q, :, A], "da", q)
            sendb[at, A] = (part[at, A] + rd[q, :, A].astype(jnp.float32)).astype(jnp.bfloat16)
            send(sendb.at[at, A], rr.at[q, 1, :, A], ("ra", q), yn)

        def pass_on_b(q):
            at, B = blk(q, 1), back_cols[q][1]
            arrive(rd.at[q, :, B], "db", q)
            sendb[at, B] = (part[at, B] + rd[q, :, B].astype(jnp.float32)).astype(jnp.bfloat16)
            send(sendb.at[at, B], rr.at[q, 0, :, B], ("rb", q), xn)

        def settle(q, cols, name, sname):
            at = blk(q, 0)
            arrive(rr.at[q, :, :, cols], name, q)
            total = part[at, cols] + rr[q, 0, :, cols].astype(jnp.float32) + rr[q, 1, :, cols].astype(jnp.float32)
            if q == p:
                part[at, cols] = total
                return
            for slot in added(q, E3_AB, I3_AB):
                arrive(zr.at[slot, :, cols], sname, slot)
                total += zr[slot, :, cols].astype(jnp.float32)
            sendb[at, cols] = total.astype(jnp.bfloat16)
            target, slot = way(q, E3_AB, I3_AB)
            send(sendb.at[at, cols], zr.at[slot, :, cols], (sname, slot), target)

        def settle_a(q):
            settle(q, back_cols[q][0], "ra", "sa")

        def settle_b(q):
            settle(q, back_cols[q][1], "rb", "sb")

        def share():
            C = back_cols[p][2]
            line_sum(p, blk(p, 0, 4), C)
            sendb[blk(p, 1, 3), C] = part[blk(p, 1, 3), C].astype(jnp.bfloat16)
            for r, other in ((1, xn), (2, yn), (3, dn)):
                place_of = xyc.at[pl.ds((r - 1) * rows, rows), pl.ds(0, C.size)]
                send(sendb.at[blk(p, r), C], place_of, ("share", 0), other)

        def close():
            at = blk(p, 0)
            for slot in added(p, E3_AB, I3_AB):
                for cols, sname in zip(back_cols[p], ("sa", "sb")):
                    arrive(zr.at[slot, :, cols], sname, slot)
                    part[at, cols] += zr[slot, :, cols].astype(jnp.float32)

        def gain():
            C = back_cols[p][2]
            arrive(xyc.at[:, pl.ds(0, C.size)], "share", 0)
            more = xyc[:, :C.size].astype(jnp.float32).reshape(3, rows, C.size)
            part[blk(p, 0), C] += more[0] + more[1] + more[2]

        def finish():
            loads[5].wait()
            total = part[blk(p, 0), :]
            factor = lax.rsqrt(jnp.mean(total * total, axis=1, keepdims=True) + norm_eps)
            post = (total * factor * post_ref[...][None]).astype(jnp.bfloat16)
            stream = stream_ref[...].astype(jnp.float32)
            out_ref[...] = (stream + post.astype(jnp.float32)).astype(jnp.bfloat16)

        def drain():
            for slot, (width, units) in enumerate(sent):
                ref = part.at[pl.ds(0, units * rows // 2), pl.ds(0, width)]
                pltpu.make_async_remote_copy(
                    src_ref=ref, dst_ref=ref, send_sem=ssem.at[slot], recv_sem=rsem.at[0],
                    device_id={"tensor": xn}, device_id_type=MESH,
                ).wait_send()

        gath[blk(p, 0), :] = normed()
        pl.semaphore_wait(barrier, 4 + p)
        programs = ((
                (start,), (relay_a, 0), (pass_a, 1), (spread, 2), (pass_b, 1), (zo, 1), (spread, 3), (pass_a, 2),
                (relay_a, 1), (zc, 1, 2), (zc, 1, 1), (relay_b, 1), (spread, 1), (relay_b, 0), (pass_b, 2),
                (zc, 1, 3), (zo, 2), (relay_a, 2), (pass_a, 3), (first, 1, 1), (zc, 2, 2), (zc, 2, 1), (relay_b, 2),
                (last, 1, 1), (pass_b, 3), (turn, 1), (out_diag, 1), (first, 0, 1), (zc, 2, 3), (zo, 3), (relay_a, 3),
                (last, 0, 1), (zc, 3, 1), (out_side, 0), (first, 2, 1), (zc, 3, 2), (relay_b, 3), (last, 2, 1),
                (zc, 3, 3), (turn, 2), (out_side, 2), (pass_on_a, 1), (out_diag, 2), (out_side, 1), (pass_on_b, 1),
                (first, 3, 1), (last, 3, 1), (out_diag, 3), (turn, 3), (pass_on_a, 2), (settle_a, 1), (pass_on_b, 2),
                (settle_b, 1), (pass_on_a, 3), (out_side, 3), (out_diag, 0), (pass_on_b, 3), (settle_b, 2),
                (settle_a, 2), (share,), (settle_a, 3), (pass_on_a, 0), (pass_on_b, 0), (settle_b, 3), (settle_a, 0),
                (gain,), (settle_b, 0), (close,), (finish,), (drain,),
            ), (
                (start,), (pass_a, 0), (relay_a, 1), (pass_a, 2), (pass_b, 0), (spread, 2), (spread, 1), (zo, 0),
                (pass_b, 2), (spread, 3), (zo, 2), (relay_a, 0), (pass_a, 3), (zc, 2, 1), (zc, 0, 2), (zc, 2, 2),
                (relay_a, 2), (relay_b, 0), (pass_b, 3), (zc, 0, 3), (zo, 3), (relay_b, 2), (zc, 2, 3), (relay_a, 3),
                (zc, 3, 1), (zc, 0, 1), (first, 0, 1), (zc, 3, 2), (last, 0, 1), (zc, 3, 3), (turn, 0), (relay_b, 3),
                (relay_b, 1), (out_diag, 0), (out_side, 0), (first, 2, 1), (last, 2, 1), (out_diag, 2), (out_side, 2),
                (first, 3, 1), (pass_on_b, 0), (last, 3, 1), (turn, 3), (out_diag, 3), (out_side, 3), (first, 1, 1),
                (pass_on_b, 2), (pass_on_a, 0), (last, 1, 1), (out_side, 1), (out_diag, 1), (pass_on_a, 2),
                (pass_on_b, 3), (turn, 2), (settle_b, 0), (settle_a, 0), (pass_on_a, 3), (pass_on_b, 1),
                (settle_a, 3), (share,), (pass_on_a, 1), (settle_b, 2), (settle_b, 3), (settle_a, 2), (settle_b, 1),
                (settle_a, 1), (gain,), (close,), (finish,), (drain,),
            ), (
                (start,), (pass_a, 2), (pass_a, 0), (relay_a, 1), (spread, 1), (spread, 2), (pass_b, 0), (pass_b, 2),
                (zo, 2), (zo, 0), (pass_a, 3), (spread, 3), (pass_b, 3), (zc, 2, 2), (zc, 2, 1), (zc, 0, 1),
                (relay_a, 0), (relay_b, 0), (zo, 3), (zc, 0, 2), (zc, 2, 3), (zc, 0, 3), (relay_b, 2), (zc, 3, 2),
                (relay_a, 3), (zc, 3, 3), (relay_b, 3), (relay_b, 1), (first, 0, 1), (relay_a, 2), (zc, 3, 1),
                (last, 0, 1), (out_diag, 0), (turn, 0), (out_side, 0), (first, 3, 1), (last, 3, 1), (turn, 3),
                (out_diag, 3), (out_side, 3), (first, 1, 1), (pass_on_a, 0), (pass_on_b, 0), (last, 1, 1),
                (out_diag, 1), (first, 2, 1), (pass_on_a, 3), (last, 2, 1), (out_diag, 2), (pass_on_b, 3),
                (out_side, 1), (turn, 2), (settle_b, 0), (out_side, 2), (settle_a, 0), (pass_on_a, 1), (pass_on_b, 1),
                (pass_on_a, 2), (settle_a, 3), (settle_b, 3), (share,), (pass_on_b, 2), (settle_b, 1), (settle_a, 1),
                (settle_a, 2), (settle_b, 2), (gain,), (close,), (finish,), (drain,),
            ), (
                (start,), (relay_a, 0), (pass_a, 1), (spread, 1), (spread, 2), (pass_b, 1), (zo, 1), (relay_b, 0),
                (pass_a, 2), (spread, 3), (zc, 1, 1), (zc, 1, 2), (relay_a, 1), (pass_b, 2), (relay_b, 1), (zo, 2),
                (first, 0, 1), (pass_a, 3), (zc, 1, 3), (relay_a, 2), (pass_b, 3), (zc, 2, 2), (relay_b, 2),
                (zc, 2, 1), (zo, 3), (first, 1, 1), (zc, 2, 3), (relay_a, 3), (last, 1, 1), (zc, 3, 2), (relay_b, 3),
                (turn, 1), (out_side, 1), (out_diag, 1), (zc, 3, 3), (first, 2, 1), (last, 2, 1), (zc, 3, 1),
                (out_diag, 2), (out_side, 2), (turn, 2), (first, 3, 1), (pass_on_b, 1), (last, 3, 1), (out_diag, 3),
                (turn, 3), (pass_on_a, 1), (pass_on_b, 2), (pass_on_a, 2), (pass_on_b, 3), (settle_b, 1),
                (settle_a, 1), (pass_on_a, 3), (out_side, 3), (settle_a, 2), (last, 0, 1), (out_diag, 0),
                (settle_b, 2), (out_side, 0), (settle_a, 3), (settle_b, 3), (pass_on_a, 0), (share,), (pass_on_b, 0),
                (settle_a, 0), (gain,), (settle_b, 0), (close,), (finish,), (drain,),
            ))
        for f, *args in programs[v]:
            with jax.named_scope("#".join([f.__name__, *map(str, args)])):
                f(*args)

    for v in range(LINE):
        pl.when(z == v)(functools.partial(run, v))


def fused(resid_stream, pre_gain, w_gate, w_up, w_down, post_gain):
    rows, d = resid_stream.shape
    ff = w_gate.shape[1]
    cw = max(cut(d, v)[1] for v in (BACK_END, BACK_MID))
    n = PLANE * LINE
    bf, f32, dma = jnp.bfloat16, jnp.float32, pltpu.SemaphoreType.DMA
    hbm = pl.BlockSpec(memory_space=pl.ANY)
    return pl.pallas_call(
        kernel,
        out_shape=pltpu.VMEM((rows, d), bf),
        in_specs=[hbm] * 6,
        out_specs=pl.BlockSpec(memory_space=pltpu.VMEM),
        scratch_shapes=[
            pltpu.VMEM((rows, d), bf),
            pltpu.VMEM((d,), f32),
            pltpu.VMEM((d,), f32),
            pltpu.VMEM((d, 2 * ff), bf),
            pltpu.VMEM((ff, d), bf),
            pltpu.VMEM((n * rows, d), bf),
            pltpu.VMEM((n * rows, 2 * ff), f32),
            pltpu.VMEM((n * rows, ff), bf),
            pltpu.VMEM((n * rows, d), f32),
            pltpu.VMEM((n * rows, d), bf),
            pltpu.VMEM((LINE, rows, d), bf),
            pltpu.VMEM((LINE, 2, rows, d), bf),
            pltpu.VMEM((WAYS, rows, d), bf),
            pltpu.VMEM((WAYS, PLANE * rows, cw), bf),
            pltpu.VMEM((3 * rows, cw), bf),
            dma((6,)),
            dma((SENDS,)),
            dma((len(ARRIVALS),)),
        ],
        compiler_params=pltpu.CompilerParams(
            collective_id=0, has_side_effects=True, vmem_limit_bytes=60 * 2**20
        ),
        name="ffn",
    )(resid_stream, pre_gain, w_gate, w_up, w_down, post_gain)


def solution(mesh):
    body = fused if mesh.shape["tensor"] == PLANE * LINE else shards
    return jax.shard_map(
        body,
        mesh=mesh,
        in_specs=(
            P(("dp", "tensor"), None),
            P(),
            P(None, "tensor"),
            P(None, "tensor"),
            P("tensor", None),
            P(),
        ),
        out_specs=P(("dp", "tensor"), None),
        check_vma=False,
    )
```

```python
import functools

import jax
import jax.numpy as jnp
from jax import lax
from jax.experimental import pallas as pl
from jax.experimental.pallas import tpu as pltpu
from jax.sharding import PartitionSpec as P

norm_eps = 1e-06
SIDE = 2
PLANE = SIDE * SIDE
OUT_END, OUT_MID, BACK_END, BACK_MID = 7, 3, 4, 4
LINE = 4
MESH = pl.DeviceIdType.MESH


def shards(resid_stream, pre_gain, w_gate, w_up, w_down, post_gain):
    stream = resid_stream.astype(jnp.float32)
    local_norm = stream * lax.rsqrt(jnp.mean(stream * stream, axis=1, keepdims=True) + norm_eps)
    normed = (local_norm * pre_gain).astype(jnp.bfloat16)
    row_piece = lax.all_gather(normed, "tensor", axis=0, tiled=True)
    gate_out = jnp.dot(row_piece, w_gate, preferred_element_type=jnp.float32)
    up_out = jnp.dot(row_piece, w_up, preferred_element_type=jnp.float32)
    hidden = (jax.nn.gelu(gate_out, approximate=True) * up_out).astype(jnp.bfloat16)
    block_rows = lax.psum_scatter(
        jnp.dot(hidden, w_down, preferred_element_type=jnp.float32),
        "tensor",
        scatter_dimension=0,
        tiled=True,
    )
    row_factor = lax.rsqrt(jnp.mean(block_rows * block_rows, axis=1, keepdims=True) + norm_eps)
    post = (block_rows * row_factor * post_gain).astype(jnp.bfloat16)
    post = lax.optimization_barrier(post)
    return (stream + post.astype(jnp.float32)).astype(jnp.bfloat16)


def cut(d, turned):
    lanes = d // 128
    most = 2 * (turned * lanes // 36) + lanes % 2
    return (lanes - most) // 2 * 128, most * 128


def parts(d, turned):
    half, cw = cut(d, turned)
    return pl.ds(0, half), pl.ds(half, half), pl.ds(2 * half, cw)


BATCH = 32
WAYS = 3
E3_AB, E3_C, I3_AB, I3_C = True, True, True, True
KIND = ("zo", "z1", "z2", "z3")
ARRIVALS = [
    *((name, q) for name in ("xa", "yb", "rest", "da", "db", "ra", "rb") for q in range(LINE)),
    *((name, j) for name in ("za", "zb", "zo", "z1", "z2", "z3") for j in range(LINE - 1)),
    *((name, i) for name in ("sa", "sb", "sc") for i in range(WAYS)),
    *(("spread", r) for r in range(1, PLANE)),
    ("share", 0),
]
SENDS = 6


def kernel(
    stream_hbm, pre_hbm, wg_hbm, wu_hbm, wd_hbm, post_hbm, out_ref,
    stream_ref, pre_ref, post_ref, w1, w2, gath, gu, hid, part, sendb, rd, rr, zr, zrc, xyc,
    lsem, ssem, rsem,
):
    rows, d = stream_ref.shape
    ff = wg_hbm.shape[1]
    group = PLANE * rows
    out_cols, back_cols = ([parts(d, v) for v in (e, m, m, e)] for e, m in ((OUT_END, OUT_MID), (BACK_END, BACK_MID)))

    me = lax.axis_index("tensor")
    x = lax.rem(me, SIDE)
    y = lax.rem(lax.div(me, SIDE), SIDE)
    z = lax.div(me, PLANE)
    sx = 1 - 2 * x
    sy = SIDE * (1 - 2 * y)
    xn, yn, dn = me + sx, me + sy, me + sx + sy
    flip = lax.div(z, LINE // 2)
    step = PLANE * (1 - 2 * flip)
    place = z + flip * (LINE - 1 - 2 * z)
    far, near = me + step, me - step

    barrier = pltpu.get_barrier_semaphore()
    for other in (xn, yn, dn, far):
        pl.semaphore_signal(barrier, inc=1, device_id={"tensor": other}, device_id_type=MESH)

    @pl.when(place == 1)
    def _():
        pl.semaphore_signal(barrier, inc=1, device_id={"tensor": near}, device_id_type=MESH)

    loads = [
        pltpu.make_async_copy(src, dst, lsem.at[i])
        for i, (src, dst) in enumerate(
            (
                (stream_hbm, stream_ref),
                (pre_hbm, pre_ref),
                (wg_hbm, w1.at[:, pl.ds(0, ff)]),
                (wu_hbm, w1.at[:, pl.ds(ff, ff)]),
                (wd_hbm, w2),
                (post_hbm, post_ref),
            )
        )
    ]
    for load in loads:
        load.start()
    loads[0].wait()
    loads[1].wait()

    def blk(q, r, n=1):
        return pl.ds((q * PLANE + r) * rows, n * rows)

    def normed():
        stream = stream_ref[...].astype(jnp.float32)
        scale = lax.rsqrt(jnp.mean(stream * stream, axis=1, keepdims=True) + norm_eps)
        return (stream * scale * pre_ref[...][None]).astype(jnp.bfloat16)

    def run(v):
        p = min(v, LINE - 1 - v)
        sent = []
        loaded, gated = set(), set()

        def send(src, dst, name, target):
            width = src.shape[-1]
            units = src.size // (rows * width) if hasattr(src, "size") else src.shape[0] // rows
            for slot, entry in enumerate(sent):
                if entry[0] == width and entry[1] + units <= BATCH:
                    entry[1] += units
                    break
            else:
                slot = len(sent)
                sent.append([width, units])
            pltpu.make_async_remote_copy(
                src_ref=src, dst_ref=dst, send_sem=ssem.at[slot], recv_sem=rsem.at[ARRIVALS.index(name)],
                device_id={"tensor": target}, device_id_type=MESH,
            ).start()

        def arrive(dst, *name):
            pltpu.make_async_remote_copy(
                src_ref=dst, dst_ref=dst, send_sem=ssem.at[0], recv_sem=rsem.at[ARRIVALS.index(name)],
                device_id={"tensor": xn}, device_id_type=MESH,
            ).wait_recv()

        def slot_of(q, owner):
            return [v for v in range(LINE) if v != owner].index(q)

        def along(at, cols, kind, q):
            ref = gath.at[at, cols]
            rel = at.start - q * group
            there = lambda v: gath.at[pl.ds(v * group + rel, at.size), cols]
            if p == 0:
                if q == 0:
                    send(ref, there(0), (kind, slot_of(0, 1)), far)
            else:
                if q in (0, 1):
                    send(ref, there(LINE - 1 - q), (kind, slot_of(LINE - 1 - q, 1)), far)
                if q in (1, 2, 3):
                    send(ref, there(q), (kind, slot_of(q, 0)), near)

        def zo(q):
            zin(q, "zo")

        def zc(q, r):
            zin(q, KIND[r])

        def zin(q, kind):
            at = blk(q, int(kind[1])) if kind[1].isdigit() else blk(q, 0)
            cols = out_cols[q][{"za": 0, "zb": 1}.get(kind, 2)]
            arrive(gath.at[at, cols], kind, slot_of(q, p))
            along(at, cols, kind, q)

        def first_a(q):
            A = out_cols[q][0]
            send(gath.at[blk(q, 0), A], gath.at[blk(q, 1), A], ("xa", q), xn)

        def first_b(q):
            B = out_cols[q][1]
            send(gath.at[blk(q, 0), B], gath.at[blk(q, 2), B], ("yb", q), yn)

        def second(q):
            A, B, _ = out_cols[q]
            send(gath.at[blk(q, 0), B], gath.at[blk(q, 1), B], ("rest", q), xn)
            send(gath.at[blk(q, 0), A], gath.at[blk(q, 2), A], ("rest", q), yn)

        def pass_a(q):
            zin(q, "za")
            first_a(q)

        def pass_b(q):
            zin(q, "zb")
            first_b(q)
            second(q)

        def relay_a(q):
            A = out_cols[q][0]
            arrive(gath.at[blk(q, 1), A], "xa", q)
            send(gath.at[blk(q, 1), A], gath.at[blk(q, 3), A], ("rest", q), yn)

        def relay_b(q):
            B = out_cols[q][1]
            arrive(gath.at[blk(q, 2), B], "yb", q)
            send(gath.at[blk(q, 2), B], gath.at[blk(q, 3), B], ("rest", q), xn)

        def start():
            A, B, C = out_cols[p]
            own = gath.at[blk(p, 0), C]
            along(blk(p, 0), A, "za", p)
            first_a(p)
            along(blk(p, 0), B, "zb", p)
            first_b(p)
            along(blk(p, 0), C, "zo", p)
            for r, other in ((1, xn), (2, yn), (3, dn)):
                send(own, gath.at[blk(p, r), C], ("spread", r), other)
            second(p)

        def spread(r):
            C = out_cols[p][2]
            arrive(gath.at[blk(p, r), C], "spread", r)
            along(blk(p, r), C, KIND[r], p)

        def full(q):
            arrive(gath.at[blk(q, 0, 4), out_cols[q][0]], "rest", q)

        def first(q, n=1):
            for v in range(q, q + n):
                full(v)
            if "in" not in loaded:
                loaded.add("in")
                loads[2].wait()
                loads[3].wait()
            beside = [v for v in (q - 1, q + 1) if n == 1 and v in gated]
            low, m = (min(q, beside[0]), 2) if beside else (q, n)
            gated.update(range(q, q + n))
            gu[blk(0, 0, m * PLANE), :] = jnp.dot(
                gath[blk(low, 0, m * PLANE), :], w1[...], preferred_element_type=jnp.float32
            )
            own = blk(q - low, 0, n * PLANE)
            gate, up = gu[own, :ff], gu[own, ff:]
            hid[blk(q, 0, n * PLANE), :] = (jax.nn.gelu(gate, approximate=True) * up).astype(jnp.bfloat16)

        def last(q, n=1):
            if "out" not in loaded:
                loaded.add("out")
                loads[4].wait()
            at = blk(q, 0, n * PLANE)

            res = jnp.dot(hid[at, :], w2[...], preferred_element_type=jnp.float32)
            part[at, :] = res
            sendb[at, :] = res.astype(jnp.bfloat16)

        def way(q, end_direct, inner_direct):
            if p == 0:
                return {1: (far, 0), 2: (far, 1), 3: (me + 3 * step, 2) if end_direct else (far, 3)}[q]
            return {0: (near, 0), 2: (far, 2), 3: (far + step, 1) if inner_direct else (far, 4)}[q]

        def added(q, end_direct, inner_direct):
            if q == p:
                return (0, 2) if p else (0, *((1,) if inner_direct else ()), *((2,) if end_direct else ()))
            if p == 0:
                return ()
            return {0: () if inner_direct else (4,), 2: (1,), 3: () if end_direct else (3,)}[q]

        def line_sum(q, at, cols):
            for slot in added(q, E3_C, I3_C):
                arrive(zrc.at[slot, :, pl.ds(0, cols.size)], "sc", slot)
                part[at, cols] += zrc[slot, :, :cols.size].astype(jnp.float32)

        def turn(q):
            at, C = blk(q, 0, 4), back_cols[q][2]
            line_sum(q, at, C)
            if added(q, E3_C, I3_C):
                sendb[at, C] = part[at, C].astype(jnp.bfloat16)
            target, slot = way(q, E3_C, I3_C)
            send(sendb.at[at, C], zrc.at[slot, :, pl.ds(0, C.size)], ("sc", slot), target)

        def out_diag(q):
            A, B, _ = back_cols[q]
            send(sendb.at[blk(q, 3), A], rd.at[q, :, A], ("da", q), xn)
            send(sendb.at[blk(q, 3), B], rd.at[q, :, B], ("db", q), yn)

        def out_side(q):
            A, B, _ = back_cols[q]
            send(sendb.at[blk(q, 1), A], rr.at[q, 0, :, A], ("ra", q), xn)
            send(sendb.at[blk(q, 2), B], rr.at[q, 1, :, B], ("rb", q), yn)

        def pass_on_a(q):
            at, A = blk(q, 2), back_cols[q][0]
            arrive(rd.at[q, :, A], "da", q)
            sendb[at, A] = (part[at, A] + rd[q, :, A].astype(jnp.float32)).astype(jnp.bfloat16)
            send(sendb.at[at, A], rr.at[q, 1, :, A], ("ra", q), yn)

        def pass_on_b(q):
            at, B = blk(q, 1), back_cols[q][1]
            arrive(rd.at[q, :, B], "db", q)
            sendb[at, B] = (part[at, B] + rd[q, :, B].astype(jnp.float32)).astype(jnp.bfloat16)
            send(sendb.at[at, B], rr.at[q, 0, :, B], ("rb", q), xn)

        def settle(q, cols, name, sname):
            at = blk(q, 0)
            arrive(rr.at[q, :, :, cols], name, q)
            total = part[at, cols] + rr[q, 0, :, cols].astype(jnp.float32) + rr[q, 1, :, cols].astype(jnp.float32)
            if q == p:
                part[at, cols] = total
                return
            for slot in added(q, E3_AB, I3_AB):
                arrive(zr.at[slot, :, cols], sname, slot)
                total += zr[slot, :, cols].astype(jnp.float32)
            sendb[at, cols] = total.astype(jnp.bfloat16)
            target, slot = way(q, E3_AB, I3_AB)
            send(sendb.at[at, cols], zr.at[slot, :, cols], (sname, slot), target)

        def settle_a(q):
            settle(q, back_cols[q][0], "ra", "sa")

        def settle_b(q):
            settle(q, back_cols[q][1], "rb", "sb")

        def share():
            C = back_cols[p][2]
            line_sum(p, blk(p, 0, 4), C)
            sendb[blk(p, 1, 3), C] = part[blk(p, 1, 3), C].astype(jnp.bfloat16)
            for r, other in ((1, xn), (2, yn), (3, dn)):
                place_of = xyc.at[pl.ds((r - 1) * rows, rows), pl.ds(0, C.size)]
                send(sendb.at[blk(p, r), C], place_of, ("share", 0), other)

        def close():
            at = blk(p, 0)
            for slot in added(p, E3_AB, I3_AB):
                for cols, sname in zip(back_cols[p], ("sa", "sb")):
                    arrive(zr.at[slot, :, cols], sname, slot)
                    part[at, cols] += zr[slot, :, cols].astype(jnp.float32)

        def gain():
            C = back_cols[p][2]
            arrive(xyc.at[:, pl.ds(0, C.size)], "share", 0)
            more = xyc[:, :C.size].astype(jnp.float32).reshape(3, rows, C.size)
            part[blk(p, 0), C] += more[0] + more[1] + more[2]

        def finish():
            loads[5].wait()
            total = part[blk(p, 0), :]
            factor = lax.rsqrt(jnp.mean(total * total, axis=1, keepdims=True) + norm_eps)
            post = (total * factor * post_ref[...][None]).astype(jnp.bfloat16)
            stream = stream_ref[...].astype(jnp.float32)
            out_ref[...] = (stream + post.astype(jnp.float32)).astype(jnp.bfloat16)

        def drain():
            for slot, (width, units) in enumerate(sent):
                ref = part.at[pl.ds(0, units * rows // 2), pl.ds(0, width)]
                pltpu.make_async_remote_copy(
                    src_ref=ref, dst_ref=ref, send_sem=ssem.at[slot], recv_sem=rsem.at[0],
                    device_id={"tensor": xn}, device_id_type=MESH,
                ).wait_send()

        gath[blk(p, 0), :] = normed()
        pl.semaphore_wait(barrier, 4 + p)
        programs = ((
                (start,), (relay_a, 0), (pass_a, 1), (spread, 2), (pass_b, 1), (zo, 1), (spread, 3), (pass_a, 2),
                (relay_a, 1), (zc, 1, 2), (zc, 1, 1), (relay_b, 1), (spread, 1), (relay_b, 0), (pass_b, 2),
                (zc, 1, 3), (zo, 2), (relay_a, 2), (pass_a, 3), (first, 1, 1), (zc, 2, 2), (zc, 2, 1), (relay_b, 2),
                (last, 1, 1), (pass_b, 3), (turn, 1), (out_diag, 1), (first, 0, 1), (zc, 2, 3), (zo, 3), (relay_a, 3),
                (last, 0, 1), (zc, 3, 1), (out_side, 0), (first, 2, 1), (zc, 3, 2), (relay_b, 3), (last, 2, 1),
                (zc, 3, 3), (turn, 2), (out_side, 2), (pass_on_a, 1), (out_diag, 2), (out_side, 1), (pass_on_b, 1),
                (first, 3, 1), (last, 3, 1), (out_diag, 3), (turn, 3), (pass_on_a, 2), (settle_a, 1), (pass_on_b, 2),
                (settle_b, 1), (pass_on_a, 3), (out_side, 3), (out_diag, 0), (pass_on_b, 3), (settle_b, 2),
                (settle_a, 2), (share,), (settle_a, 3), (pass_on_a, 0), (pass_on_b, 0), (settle_b, 3), (settle_a, 0),
                (gain,), (settle_b, 0), (close,), (finish,), (drain,),
            ), (
                (start,), (pass_a, 0), (relay_a, 1), (pass_a, 2), (pass_b, 0), (spread, 2), (spread, 1), (zo, 0),
                (pass_b, 2), (spread, 3), (zo, 2), (relay_a, 0), (pass_a, 3), (zc, 2, 1), (zc, 0, 2), (zc, 2, 2),
                (relay_a, 2), (relay_b, 0), (pass_b, 3), (zc, 0, 3), (zo, 3), (relay_b, 2), (zc, 2, 3), (relay_a, 3),
                (zc, 3, 1), (zc, 0, 1), (first, 0, 1), (zc, 3, 2), (last, 0, 1), (zc, 3, 3), (turn, 0), (relay_b, 3),
                (relay_b, 1), (out_diag, 0), (out_side, 0), (first, 2, 1), (last, 2, 1), (out_diag, 2), (out_side, 2),
                (first, 3, 1), (pass_on_b, 0), (last, 3, 1), (turn, 3), (out_diag, 3), (out_side, 3), (first, 1, 1),
                (pass_on_b, 2), (pass_on_a, 0), (last, 1, 1), (out_side, 1), (out_diag, 1), (pass_on_a, 2),
                (pass_on_b, 3), (turn, 2), (settle_b, 0), (settle_a, 0), (pass_on_a, 3), (pass_on_b, 1),
                (settle_a, 3), (share,), (pass_on_a, 1), (settle_b, 2), (settle_b, 3), (settle_a, 2), (settle_b, 1),
                (settle_a, 1), (gain,), (close,), (finish,), (drain,),
            ), (
                (start,), (pass_a, 2), (pass_a, 0), (relay_a, 1), (spread, 1), (spread, 2), (pass_b, 0), (pass_b, 2),
                (zo, 2), (zo, 0), (pass_a, 3), (spread, 3), (pass_b, 3), (zc, 2, 2), (zc, 2, 1), (zc, 0, 1),
                (relay_a, 0), (relay_b, 0), (zo, 3), (zc, 0, 2), (zc, 2, 3), (zc, 0, 3), (relay_b, 2), (zc, 3, 2),
                (relay_a, 3), (zc, 3, 3), (relay_b, 3), (relay_b, 1), (first, 0, 1), (relay_a, 2), (zc, 3, 1),
                (last, 0, 1), (out_diag, 0), (turn, 0), (out_side, 0), (first, 3, 1), (last, 3, 1), (turn, 3),
                (out_diag, 3), (out_side, 3), (first, 1, 1), (pass_on_a, 0), (pass_on_b, 0), (last, 1, 1),
                (out_diag, 1), (first, 2, 1), (pass_on_a, 3), (last, 2, 1), (out_diag, 2), (pass_on_b, 3),
                (out_side, 1), (turn, 2), (settle_b, 0), (out_side, 2), (settle_a, 0), (pass_on_a, 1), (pass_on_b, 1),
                (pass_on_a, 2), (settle_a, 3), (settle_b, 3), (share,), (pass_on_b, 2), (settle_b, 1), (settle_a, 1),
                (settle_a, 2), (settle_b, 2), (gain,), (close,), (finish,), (drain,),
            ), (
                (start,), (relay_a, 0), (pass_a, 1), (spread, 1), (spread, 2), (pass_b, 1), (zo, 1), (relay_b, 0),
                (pass_a, 2), (spread, 3), (zc, 1, 1), (zc, 1, 2), (relay_a, 1), (pass_b, 2), (relay_b, 1), (zo, 2),
                (first, 0, 1), (pass_a, 3), (zc, 1, 3), (relay_a, 2), (pass_b, 3), (zc, 2, 2), (relay_b, 2),
                (zc, 2, 1), (zo, 3), (first, 1, 1), (zc, 2, 3), (relay_a, 3), (last, 1, 1), (zc, 3, 2), (relay_b, 3),
                (turn, 1), (out_side, 1), (out_diag, 1), (zc, 3, 3), (first, 2, 1), (last, 2, 1), (zc, 3, 1),
                (out_diag, 2), (out_side, 2), (turn, 2), (first, 3, 1), (pass_on_b, 1), (last, 3, 1), (out_diag, 3),
                (turn, 3), (pass_on_a, 1), (pass_on_b, 2), (pass_on_a, 2), (pass_on_b, 3), (settle_b, 1),
                (settle_a, 1), (pass_on_a, 3), (out_side, 3), (settle_a, 2), (last, 0, 1), (out_diag, 0),
                (settle_b, 2), (out_side, 0), (settle_a, 3), (settle_b, 3), (pass_on_a, 0), (share,), (pass_on_b, 0),
                (settle_a, 0), (gain,), (settle_b, 0), (close,), (finish,), (drain,),
            ))
        for f, *args in programs[v]:
            with jax.named_scope("#".join([f.__name__, *map(str, args)])):
                f(*args)

    for v in reversed(range(LINE)):
        pl.when(z == v)(functools.partial(run, v))


def fused(resid_stream, pre_gain, w_gate, w_up, w_down, post_gain):
    rows, d = resid_stream.shape
    ff = w_gate.shape[1]
    cw = max(cut(d, v)[1] for v in (BACK_END, BACK_MID))
    n = PLANE * LINE
    bf, f32, dma = jnp.bfloat16, jnp.float32, pltpu.SemaphoreType.DMA
    hbm = pl.BlockSpec(memory_space=pl.ANY)
    return pl.pallas_call(
        kernel,
        out_shape=pltpu.VMEM((rows, d), bf),
        in_specs=[hbm] * 6,
        out_specs=pl.BlockSpec(memory_space=pltpu.VMEM),
        scratch_shapes=[
            pltpu.VMEM((rows, d), bf),
            pltpu.VMEM((d,), f32),
            pltpu.VMEM((d,), f32),
            pltpu.VMEM((d, 2 * ff), bf),
            pltpu.VMEM((ff, d), bf),
            pltpu.VMEM((n * rows, d), bf),
            pltpu.VMEM((n * rows, 2 * ff), f32),
            pltpu.VMEM((n * rows, ff), bf),
            pltpu.VMEM((n * rows, d), f32),
            pltpu.VMEM((n * rows, d), bf),
            pltpu.VMEM((LINE, rows, d), bf),
            pltpu.VMEM((LINE, 2, rows, d), bf),
            pltpu.VMEM((WAYS, rows, d), bf),
            pltpu.VMEM((WAYS, PLANE * rows, cw), bf),
            pltpu.VMEM((3 * rows, cw), bf),
            dma((6,)),
            dma((SENDS,)),
            dma((len(ARRIVALS),)),
        ],
        compiler_params=pltpu.CompilerParams(
            collective_id=0, has_side_effects=True, vmem_limit_bytes=60 * 2**20
        ),
        name="ffn",
    )(resid_stream, pre_gain, w_gate, w_up, w_down, post_gain)


def solution(mesh):
    body = fused if mesh.shape["tensor"] == PLANE * LINE else shards
    return jax.shard_map(
        body,
        mesh=mesh,
        in_specs=(
            P(("dp", "tensor"), None),
            P(),
            P(None, "tensor"),
            P(None, "tensor"),
            P("tensor", None),
            P(),
        ),
        out_specs=P(("dp", "tensor"), None),
        check_vma=False,
    )
```

```python
import functools

import jax
import jax.numpy as jnp
from jax import lax
from jax.experimental import pallas as pl
from jax.experimental.pallas import tpu as pltpu
from jax.sharding import PartitionSpec as P

norm_eps = 1e-06
SIDE = 2
PLANE = SIDE * SIDE
OUT_END, OUT_MID, BACK_END, BACK_MID = 8, 3, 4, 4
LINE = 4
MESH = pl.DeviceIdType.MESH


def shards(resid_stream, pre_gain, w_gate, w_up, w_down, post_gain):
    stream = resid_stream.astype(jnp.float32)
    local_norm = stream * lax.rsqrt(jnp.mean(stream * stream, axis=1, keepdims=True) + norm_eps)
    normed = (local_norm * pre_gain).astype(jnp.bfloat16)
    row_piece = lax.all_gather(normed, "tensor", axis=0, tiled=True)
    gate_out = jnp.dot(row_piece, w_gate, preferred_element_type=jnp.float32)
    up_out = jnp.dot(row_piece, w_up, preferred_element_type=jnp.float32)
    hidden = (jax.nn.gelu(gate_out, approximate=True) * up_out).astype(jnp.bfloat16)
    block_rows = lax.psum_scatter(
        jnp.dot(hidden, w_down, preferred_element_type=jnp.float32),
        "tensor",
        scatter_dimension=0,
        tiled=True,
    )
    row_factor = lax.rsqrt(jnp.mean(block_rows * block_rows, axis=1, keepdims=True) + norm_eps)
    post = (block_rows * row_factor * post_gain).astype(jnp.bfloat16)
    post = lax.optimization_barrier(post)
    return (stream + post.astype(jnp.float32)).astype(jnp.bfloat16)


def cut(d, turned):
    lanes = d // 128
    most = 2 * (turned * lanes // 36) + lanes % 2
    return (lanes - most) // 2 * 128, most * 128


def parts(d, turned):
    half, cw = cut(d, turned)
    return pl.ds(0, half), pl.ds(half, half), pl.ds(2 * half, cw)


BATCH = 32
WAYS = 3
E3_AB, E3_C, I3_AB, I3_C = True, True, True, True
KIND = ("zo", "z1", "z2", "z3")
ARRIVALS = [
    *((name, q) for name in ("xa", "yb", "rest", "da", "db", "ra", "rb") for q in range(LINE)),
    *((name, j) for name in ("za", "zb", "zo", "z1", "z2", "z3") for j in range(LINE - 1)),
    *((name, i) for name in ("sa", "sb", "sc") for i in range(WAYS)),
    *(("spread", r) for r in range(1, PLANE)),
    ("share", 0),
]
SENDS = 6


def kernel(
    stream_hbm, pre_hbm, wg_hbm, wu_hbm, wd_hbm, post_hbm, out_ref,
    stream_ref, pre_ref, post_ref, w1, w2, gath, gu, hid, part, sendb, rd, rr, zr, zrc, xyc,
    lsem, ssem, rsem,
):
    rows, d = stream_ref.shape
    ff = wg_hbm.shape[1]
    group = PLANE * rows
    out_cols, back_cols = ([parts(d, v) for v in (e, m, m, e)] for e, m in ((OUT_END, OUT_MID), (BACK_END, BACK_MID)))

    me = lax.axis_index("tensor")
    x = lax.rem(me, SIDE)
    y = lax.rem(lax.div(me, SIDE), SIDE)
    z = lax.div(me, PLANE)
    sx = 1 - 2 * x
    sy = SIDE * (1 - 2 * y)
    xn, yn, dn = me + sx, me + sy, me + sx + sy
    flip = lax.div(z, LINE // 2)
    step = PLANE * (1 - 2 * flip)
    place = z + flip * (LINE - 1 - 2 * z)
    far, near = me + step, me - step

    barrier = pltpu.get_barrier_semaphore()
    for other in (xn, yn, dn, far):
        pl.semaphore_signal(barrier, inc=1, device_id={"tensor": other}, device_id_type=MESH)

    @pl.when(place == 1)
    def _():
        pl.semaphore_signal(barrier, inc=1, device_id={"tensor": near}, device_id_type=MESH)

    loads = [
        pltpu.make_async_copy(src, dst, lsem.at[i])
        for i, (src, dst) in enumerate(
            (
                (stream_hbm, stream_ref),
                (pre_hbm, pre_ref),
                (wg_hbm, w1.at[:, pl.ds(0, ff)]),
                (wu_hbm, w1.at[:, pl.ds(ff, ff)]),
                (wd_hbm, w2),
                (post_hbm, post_ref),
            )
        )
    ]
    for load in loads:
        load.start()
    loads[0].wait()
    loads[1].wait()

    def blk(q, r, n=1):
        return pl.ds((q * PLANE + r) * rows, n * rows)

    def normed():
        stream = stream_ref[...].astype(jnp.float32)
        scale = lax.rsqrt(jnp.mean(stream * stream, axis=1, keepdims=True) + norm_eps)
        return (stream * scale * pre_ref[...][None]).astype(jnp.bfloat16)

    def run(v):
        p = min(v, LINE - 1 - v)
        sent = []
        loaded, gated = set(), set()

        def send(src, dst, name, target):
            width = src.shape[-1]
            units = src.size // (rows * width) if hasattr(src, "size") else src.shape[0] // rows
            for slot, entry in enumerate(sent):
                if entry[0] == width and entry[1] + units <= BATCH:
                    entry[1] += units
                    break
            else:
                slot = len(sent)
                sent.append([width, units])
            pltpu.make_async_remote_copy(
                src_ref=src, dst_ref=dst, send_sem=ssem.at[slot], recv_sem=rsem.at[ARRIVALS.index(name)],
                device_id={"tensor": target}, device_id_type=MESH,
            ).start()

        def arrive(dst, *name):
            pltpu.make_async_remote_copy(
                src_ref=dst, dst_ref=dst, send_sem=ssem.at[0], recv_sem=rsem.at[ARRIVALS.index(name)],
                device_id={"tensor": xn}, device_id_type=MESH,
            ).wait_recv()

        def slot_of(q, owner):
            return [v for v in range(LINE) if v != owner].index(q)

        def along(at, cols, kind, q):
            ref = gath.at[at, cols]
            rel = at.start - q * group
            there = lambda v: gath.at[pl.ds(v * group + rel, at.size), cols]
            if p == 0:
                if q == 0:
                    send(ref, there(0), (kind, slot_of(0, 1)), far)
            else:
                if q in (0, 1):
                    send(ref, there(LINE - 1 - q), (kind, slot_of(LINE - 1 - q, 1)), far)
                if q in (1, 2, 3):
                    send(ref, there(q), (kind, slot_of(q, 0)), near)

        def zo(q):
            zin(q, "zo")

        def zc(q, r):
            zin(q, KIND[r])

        def zin(q, kind):
            at = blk(q, int(kind[1])) if kind[1].isdigit() else blk(q, 0)
            cols = out_cols[q][{"za": 0, "zb": 1}.get(kind, 2)]
            arrive(gath.at[at, cols], kind, slot_of(q, p))
            along(at, cols, kind, q)

        def first_a(q):
            A = out_cols[q][0]
            send(gath.at[blk(q, 0), A], gath.at[blk(q, 1), A], ("xa", q), xn)

        def first_b(q):
            B = out_cols[q][1]
            send(gath.at[blk(q, 0), B], gath.at[blk(q, 2), B], ("yb", q), yn)

        def second(q):
            A, B, _ = out_cols[q]
            send(gath.at[blk(q, 0), B], gath.at[blk(q, 1), B], ("rest", q), xn)
            send(gath.at[blk(q, 0), A], gath.at[blk(q, 2), A], ("rest", q), yn)

        def pass_a(q):
            zin(q, "za")
            first_a(q)

        def pass_b(q):
            zin(q, "zb")
            first_b(q)
            second(q)

        def relay_a(q):
            A = out_cols[q][0]
            arrive(gath.at[blk(q, 1), A], "xa", q)
            send(gath.at[blk(q, 1), A], gath.at[blk(q, 3), A], ("rest", q), yn)

        def relay_b(q):
            B = out_cols[q][1]
            arrive(gath.at[blk(q, 2), B], "yb", q)
            send(gath.at[blk(q, 2), B], gath.at[blk(q, 3), B], ("rest", q), xn)

        def start():
            A, B, C = out_cols[p]
            own = gath.at[blk(p, 0), C]
            along(blk(p, 0), A, "za", p)
            first_a(p)
            along(blk(p, 0), B, "zb", p)
            first_b(p)
            along(blk(p, 0), C, "zo", p)
            for r, other in ((1, xn), (2, yn), (3, dn)):
                send(own, gath.at[blk(p, r), C], ("spread", r), other)
            second(p)

        def spread(r):
            C = out_cols[p][2]
            arrive(gath.at[blk(p, r), C], "spread", r)
            along(blk(p, r), C, KIND[r], p)

        def full(q):
            arrive(gath.at[blk(q, 0, 4), out_cols[q][0]], "rest", q)

        def first(q, n=1):
            for v in range(q, q + n):
                full(v)
            if "in" not in loaded:
                loaded.add("in")
                loads[2].wait()
                loads[3].wait()
            beside = [v for v in (q - 1, q + 1) if n == 1 and v in gated]
            low, m = (min(q, beside[0]), 2) if beside else (q, n)
            gated.update(range(q, q + n))
            gu[blk(0, 0, m * PLANE), :] = jnp.dot(
                gath[blk(low, 0, m * PLANE), :], w1[...], preferred_element_type=jnp.float32
            )
            own = blk(q - low, 0, n * PLANE)
            gate, up = gu[own, :ff], gu[own, ff:]
            hid[blk(q, 0, n * PLANE), :] = (jax.nn.gelu(gate, approximate=True) * up).astype(jnp.bfloat16)

        def last(q, n=1):
            if "out" not in loaded:
                loaded.add("out")
                loads[4].wait()
            at = blk(q, 0, n * PLANE)

            res = jnp.dot(hid[at, :], w2[...], preferred_element_type=jnp.float32)
            part[at, :] = res
            sendb[at, :] = res.astype(jnp.bfloat16)

        def way(q, end_direct, inner_direct):
            if p == 0:
                return {1: (far, 0), 2: (far, 1), 3: (me + 3 * step, 2) if end_direct else (far, 3)}[q]
            return {0: (near, 0), 2: (far, 2), 3: (far + step, 1) if inner_direct else (far, 4)}[q]

        def added(q, end_direct, inner_direct):
            if q == p:
                return (0, 2) if p else (0, *((1,) if inner_direct else ()), *((2,) if end_direct else ()))
            if p == 0:
                return ()
            return {0: () if inner_direct else (4,), 2: (1,), 3: () if end_direct else (3,)}[q]

        def line_sum(q, at, cols):
            for slot in added(q, E3_C, I3_C):
                arrive(zrc.at[slot, :, pl.ds(0, cols.size)], "sc", slot)
                part[at, cols] += zrc[slot, :, :cols.size].astype(jnp.float32)

        def turn(q):
            at, C = blk(q, 0, 4), back_cols[q][2]
            line_sum(q, at, C)
            if added(q, E3_C, I3_C):
                sendb[at, C] = part[at, C].astype(jnp.bfloat16)
            target, slot = way(q, E3_C, I3_C)
            send(sendb.at[at, C], zrc.at[slot, :, pl.ds(0, C.size)], ("sc", slot), target)

        def out_diag(q):
            A, B, _ = back_cols[q]
            send(sendb.at[blk(q, 3), A], rd.at[q, :, A], ("da", q), xn)
            send(sendb.at[blk(q, 3), B], rd.at[q, :, B], ("db", q), yn)

        def out_side(q):
            A, B, _ = back_cols[q]
            send(sendb.at[blk(q, 1), A], rr.at[q, 0, :, A], ("ra", q), xn)
            send(sendb.at[blk(q, 2), B], rr.at[q, 1, :, B], ("rb", q), yn)

        def pass_on_a(q):
            at, A = blk(q, 2), back_cols[q][0]
            arrive(rd.at[q, :, A], "da", q)
            sendb[at, A] = (part[at, A] + rd[q, :, A].astype(jnp.float32)).astype(jnp.bfloat16)
            send(sendb.at[at, A], rr.at[q, 1, :, A], ("ra", q), yn)

        def pass_on_b(q):
            at, B = blk(q, 1), back_cols[q][1]
            arrive(rd.at[q, :, B], "db", q)
            sendb[at, B] = (part[at, B] + rd[q, :, B].astype(jnp.float32)).astype(jnp.bfloat16)
            send(sendb.at[at, B], rr.at[q, 0, :, B], ("rb", q), xn)

        def settle(q, cols, name, sname):
            at = blk(q, 0)
            arrive(rr.at[q, :, :, cols], name, q)
            total = part[at, cols] + rr[q, 0, :, cols].astype(jnp.float32) + rr[q, 1, :, cols].astype(jnp.float32)
            if q == p:
                part[at, cols] = total
                return
            for slot in added(q, E3_AB, I3_AB):
                arrive(zr.at[slot, :, cols], sname, slot)
                total += zr[slot, :, cols].astype(jnp.float32)
            sendb[at, cols] = total.astype(jnp.bfloat16)
            target, slot = way(q, E3_AB, I3_AB)
            send(sendb.at[at, cols], zr.at[slot, :, cols], (sname, slot), target)

        def settle_a(q):
            settle(q, back_cols[q][0], "ra", "sa")

        def settle_b(q):
            settle(q, back_cols[q][1], "rb", "sb")

        def share():
            C = back_cols[p][2]
            line_sum(p, blk(p, 0, 4), C)
            sendb[blk(p, 1, 3), C] = part[blk(p, 1, 3), C].astype(jnp.bfloat16)
            for r, other in ((1, xn), (2, yn), (3, dn)):
                place_of = xyc.at[pl.ds((r - 1) * rows, rows), pl.ds(0, C.size)]
                send(sendb.at[blk(p, r), C], place_of, ("share", 0), other)

        def close():
            at = blk(p, 0)
            for slot in added(p, E3_AB, I3_AB):
                for cols, sname in zip(back_cols[p], ("sa", "sb")):
                    arrive(zr.at[slot, :, cols], sname, slot)
                    part[at, cols] += zr[slot, :, cols].astype(jnp.float32)

        def gain():
            C = back_cols[p][2]
            arrive(xyc.at[:, pl.ds(0, C.size)], "share", 0)
            more = xyc[:, :C.size].astype(jnp.float32).reshape(3, rows, C.size)
            part[blk(p, 0), C] += more[0] + more[1] + more[2]

        def finish():
            loads[5].wait()
            total = part[blk(p, 0), :]
            factor = lax.rsqrt(jnp.mean(total * total, axis=1, keepdims=True) + norm_eps)
            post = (total * factor * post_ref[...][None]).astype(jnp.bfloat16)
            stream = stream_ref[...].astype(jnp.float32)
            out_ref[...] = (stream + post.astype(jnp.float32)).astype(jnp.bfloat16)

        def drain():
            for slot, (width, units) in enumerate(sent):
                ref = part.at[pl.ds(0, units * rows // 2), pl.ds(0, width)]
                pltpu.make_async_remote_copy(
                    src_ref=ref, dst_ref=ref, send_sem=ssem.at[slot], recv_sem=rsem.at[0],
                    device_id={"tensor": xn}, device_id_type=MESH,
                ).wait_send()

        gath[blk(p, 0), :] = normed()
        pl.semaphore_wait(barrier, 4 + p)
        programs = ((
                (start,), (relay_a, 0), (relay_b, 0), (pass_a, 1), (spread, 1), (spread, 2), (pass_b, 1), (zo, 1),
                (pass_a, 2), (spread, 3), (relay_b, 1), (zc, 1, 2), (relay_a, 1), (pass_b, 2), (zc, 1, 3), (zo, 2),
                (relay_a, 2), (pass_a, 3), (zc, 2, 1), (first, 0, 1), (zc, 1, 1), (relay_b, 2), (zc, 2, 2),
                (pass_b, 3), (first, 1, 1), (zo, 3), (last, 1, 1), (relay_a, 3), (zc, 2, 3), (turn, 1), (out_diag, 1),
                (last, 0, 1), (out_side, 0), (zc, 3, 1), (relay_b, 3), (first, 2, 1), (zc, 3, 2), (last, 2, 1),
                (out_diag, 2), (turn, 2), (out_side, 2), (pass_on_a, 1), (zc, 3, 3), (pass_on_b, 1), (first, 3, 1),
                (pass_on_b, 2), (pass_on_a, 2), (last, 3, 1), (turn, 3), (out_diag, 3), (out_side, 3), (settle_a, 2),
                (settle_b, 2), (pass_on_b, 3), (pass_on_a, 3), (out_diag, 0), (out_side, 1), (share,), (settle_b, 3),
                (settle_a, 3), (pass_on_a, 0), (pass_on_b, 0), (settle_a, 1), (settle_b, 1), (settle_a, 0),
                (settle_b, 0), (gain,), (close,), (finish,), (drain,),
            ), (
                (start,), (pass_a, 0), (relay_a, 1), (relay_b, 1), (pass_b, 0), (pass_a, 2), (spread, 1), (spread, 2),
                (zo, 0), (pass_b, 2), (pass_a, 3), (spread, 3), (zo, 2), (relay_a, 0), (zc, 2, 1), (zc, 2, 2),
                (zc, 0, 1), (first, 1, 1), (zc, 0, 2), (relay_b, 0), (pass_b, 3), (last, 1, 1), (zo, 3), (relay_a, 2),
                (out_diag, 1), (relay_b, 2), (zc, 2, 3), (zc, 0, 3), (zc, 3, 1), (relay_a, 3), (zc, 3, 2),
                (relay_b, 3), (first, 0, 1), (last, 0, 1), (zc, 3, 3), (out_diag, 0), (out_side, 0), (turn, 0),
                (first, 2, 1), (pass_on_b, 1), (pass_on_a, 1), (last, 2, 1), (out_diag, 2), (out_side, 2),
                (first, 3, 1), (last, 3, 1), (turn, 3), (out_diag, 3), (pass_on_b, 0), (out_side, 3), (pass_on_a, 0),
                (pass_on_b, 2), (out_side, 1), (pass_on_a, 2), (turn, 2), (pass_on_b, 3), (pass_on_a, 3),
                (settle_b, 0), (settle_a, 0), (settle_b, 1), (settle_a, 2), (settle_a, 3), (settle_b, 3),
                (settle_a, 1), (settle_b, 2), (share,), (gain,), (close,), (finish,), (drain,),
            ), (
                (start,), (pass_a, 2), (pass_a, 0), (relay_a, 1), (spread, 1), (spread, 2), (pass_b, 0), (pass_b, 2),
                (zo, 0), (pass_a, 3), (zo, 2), (spread, 3), (pass_b, 3), (zc, 2, 1), (zc, 2, 2), (relay_a, 0),
                (relay_b, 0), (zc, 0, 1), (zo, 3), (zc, 2, 3), (zc, 0, 2), (relay_b, 2), (zc, 3, 1), (relay_a, 3),
                (zc, 0, 3), (relay_b, 3), (relay_b, 1), (zc, 3, 2), (zc, 3, 3), (first, 0, 1), (relay_a, 2),
                (last, 0, 1), (out_side, 0), (out_diag, 0), (turn, 0), (first, 3, 1), (last, 3, 1), (out_diag, 3),
                (out_side, 3), (turn, 3), (first, 1, 1), (first, 2, 1), (pass_on_a, 0), (pass_on_b, 0), (last, 2, 1),
                (out_diag, 2), (pass_on_a, 3), (out_side, 2), (last, 1, 1), (pass_on_b, 3), (out_diag, 1),
                (out_side, 1), (turn, 2), (settle_a, 0), (settle_b, 0), (pass_on_b, 2), (pass_on_a, 2), (settle_a, 3),
                (settle_b, 3), (share,), (pass_on_b, 1), (pass_on_a, 1), (settle_a, 2), (settle_b, 2), (settle_a, 1),
                (gain,), (settle_b, 1), (close,), (finish,), (drain,),
            ), (
                (start,), (relay_a, 0), (pass_a, 1), (spread, 1), (spread, 2), (pass_b, 1), (zo, 1), (relay_b, 0),
                (pass_a, 2), (zc, 1, 1), (zc, 1, 2), (spread, 3), (relay_a, 1), (pass_b, 2), (relay_b, 1),
                (first, 0, 1), (zo, 2), (pass_a, 3), (pass_b, 3), (relay_a, 2), (zc, 1, 3), (zc, 2, 1), (zc, 2, 2),
                (relay_b, 2), (zo, 3), (first, 1, 1), (zc, 2, 3), (relay_b, 3), (relay_a, 3), (last, 1, 1),
                (out_side, 1), (zc, 3, 1), (turn, 1), (out_diag, 1), (first, 2, 1), (zc, 3, 2), (last, 2, 1),
                (out_diag, 2), (turn, 2), (out_side, 2), (zc, 3, 3), (first, 3, 1), (last, 3, 1), (pass_on_b, 1),
                (out_diag, 3), (turn, 3), (pass_on_a, 1), (pass_on_a, 2), (pass_on_b, 2), (settle_b, 1),
                (pass_on_b, 3), (pass_on_a, 3), (out_side, 3), (settle_a, 1), (settle_a, 2), (settle_b, 2),
                (last, 0, 1), (out_diag, 0), (out_side, 0), (settle_a, 3), (settle_b, 3), (pass_on_a, 0),
                (pass_on_b, 0), (share,), (settle_a, 0), (settle_b, 0), (gain,), (close,), (finish,), (drain,),
            ))
        for f, *args in programs[v]:
            with jax.named_scope("#".join([f.__name__, *map(str, args)])):
                f(*args)

    for v in reversed(range(LINE)):
        pl.when(z == v)(functools.partial(run, v))


def fused(resid_stream, pre_gain, w_gate, w_up, w_down, post_gain):
    rows, d = resid_stream.shape
    ff = w_gate.shape[1]
    cw = max(cut(d, v)[1] for v in (BACK_END, BACK_MID))
    n = PLANE * LINE
    bf, f32, dma = jnp.bfloat16, jnp.float32, pltpu.SemaphoreType.DMA
    hbm = pl.BlockSpec(memory_space=pl.ANY)
    return pl.pallas_call(
        kernel,
        out_shape=pltpu.VMEM((rows, d), bf),
        in_specs=[hbm] * 6,
        out_specs=pl.BlockSpec(memory_space=pltpu.VMEM),
        scratch_shapes=[
            pltpu.VMEM((rows, d), bf),
            pltpu.VMEM((d,), f32),
            pltpu.VMEM((d,), f32),
            pltpu.VMEM((d, 2 * ff), bf),
            pltpu.VMEM((ff, d), bf),
            pltpu.VMEM((n * rows, d), bf),
            pltpu.VMEM((n * rows, 2 * ff), f32),
            pltpu.VMEM((n * rows, ff), bf),
            pltpu.VMEM((n * rows, d), f32),
            pltpu.VMEM((n * rows, d), bf),
            pltpu.VMEM((LINE, rows, d), bf),
            pltpu.VMEM((LINE, 2, rows, d), bf),
            pltpu.VMEM((WAYS, rows, d), bf),
            pltpu.VMEM((WAYS, PLANE * rows, cw), bf),
            pltpu.VMEM((3 * rows, cw), bf),
            dma((6,)),
            dma((SENDS,)),
            dma((len(ARRIVALS),)),
        ],
        compiler_params=pltpu.CompilerParams(
            collective_id=0, has_side_effects=True, vmem_limit_bytes=60 * 2**20
        ),
        name="ffn",
    )(resid_stream, pre_gain, w_gate, w_up, w_down, post_gain)


def solution(mesh):
    body = fused if mesh.shape["tensor"] == PLANE * LINE else shards
    return jax.shard_map(
        body,
        mesh=mesh,
        in_specs=(
            P(("dp", "tensor"), None),
            P(),
            P(None, "tensor"),
            P(None, "tensor"),
            P("tensor", None),
            P(),
        ),
        out_specs=P(("dp", "tensor"), None),
        check_vma=False,
    )
```
